128 devices in a mesh: wide: 16 (over z, x_lo, core), narrow: 8 (over y, x_hi).
Axes of the slice: x: 4 (x_hi: 2, x_lo: 2; x = x_hi * 2 + x_lo), y: 4, z: 4, core: 2. Of those that a mesh axis runs over, the one named last changes fastest.
Arguments:
- offsets: float32 [2, 16, 8, 8192], P(None, 'wide', 'narrow'), may hold values from -1 to 1
- strengths: float32 [2, 16, 8, 8192], P(None, 'wide', 'narrow'), may hold values from -1.2 to 1.2
- leaf_map: int32 [16, 8, 8192], P('wide', 'narrow'), may hold values from 0 to 1023
- shift_matrices: float32 [7, 4, 128, 128], replicated, may hold values from -0.25 to 0.25
- transfer_diagonal: float32 [5, 49, 128], replicated, may hold values from -1.25 to 1.25
Outputs:
- leaf_multipoles: float32 [512, 256, 128], P('wide', 'narrow')
- local_zero: float32 [16, 8, 128], P('wide', 'narrow')
- local_one: float32 [32, 16, 128], P('wide', 'narrow')
- local_two: float32 [64, 32, 128], P('wide', 'narrow')
- local_three: float32 [128, 64, 128], P('wide', 'narrow')
- coarse_local: float32 [8, 4, 128], replicated
- top_multipole: float32 [4, 2, 128], replicated
The draws below stay inside these ranges and needn't reach their ends.
All inputs are finite; a program needn't handle non-finite values.
Results may differ from the reference program's by a relative error of at most 0.0003.
Values sent between devices are 32-bit elements; how exact they have to be, the bound alone decides.
No kernel may reach another device: no remote copies, remote signals or barrier semaphores. Data moves between devices by JAX's collectives and lax.ppermute only.
A program may use at most 128 MiB of HBM per device.

```python
import math
import jax
import jax.numpy as jnp
from jax import lax

ORDER = 64
COEFFS = 128
LOCAL = 5
COARSE = 2
LEAF_SIDE = 32
TRANSFER_LEVELS = 5
PAN_DEV = 8192
N_WIDE = 16
N_NARROW = 8


def set_ends(drawn, key, low, top_value):
    longest = drawn.shape.index(max(drawn.shape))
    spots = []
    for shift in (0, 1):
        where = [jax.random.randint(jax.random.fold_in(key, axis), (), 0, length) for axis, length in enumerate(drawn.shape)]
        where[longest] = (where[longest] + shift) % drawn.shape[longest]
        spots.append(tuple(where))
    return drawn.at[spots[0]].set(low).at[spots[1]].set(top_value)


def shard_levels(stream_key, shape, split, low, high):
    gain, own = 1.0, jax.random.fold_in(stream_key, 6)
    for position, blocks in split:
        steps = jnp.exp(jax.random.uniform(jax.random.fold_in(own, position), (blocks,), jnp.float32, low / len(split), high / len(split)))
        gain = gain * jnp.repeat(steps, shape[position] // blocks).reshape([-1 if axis == position else 1 for axis in range(len(shape))])
    return gain


def centred(key, dims, scale, reach, cuts=(), held_as=jnp.bfloat16):
    entries = jax.random.normal(key, dims, jnp.float32) * scale
    if len(cuts) > 0:
        entries = shard_levels(key, dims, cuts, -0.22, 0.18) * entries
    return jnp.clip(entries, min=-reach, max=reach).astype(held_as)


def setup_inputs(seed: int = 0) -> dict:
    splits = jax.random.split(jax.random.key(seed), 6)
    return {
        "offsets": jnp.clip(jax.random.uniform(splits[0], (2, N_WIDE, N_NARROW, PAN_DEV), jnp.float32, -1.0, 1.0) * shard_levels(splits[0], (2, N_WIDE, N_NARROW, PAN_DEV), ((1, 16), (2, 8)), -0.4, 0.0), -1.0, 1.0),
        "strengths": centred(splits[1], (2, N_WIDE, N_NARROW, PAN_DEV), 0.2, 1.2, ((1, 16), (2, 8)), jnp.float32),
        "leaf_map": set_ends(jax.random.randint(splits[2], (N_WIDE, N_NARROW, PAN_DEV), 0, LEAF_SIDE * LEAF_SIDE), jax.random.fold_in(splits[2], 1), 0, (LEAF_SIDE * LEAF_SIDE) - 1).astype(jnp.int32),
        "shift_matrices": centred(splits[3], (LOCAL + COARSE, 4, COEFFS, COEFFS), (4 * COEFFS) ** -0.5, 0.25, (), jnp.float32),
        "transfer_diagonal": centred(splits[4], (TRANSFER_LEVELS, 49, COEFFS), 0.2, 1.25, (), jnp.float32),
    }


HIGHEST = lax.Precision.HIGHEST


def panel_terms(coords, charge):
    degree = jnp.arange(ORDER).astype(jnp.float32)
    cheb_first = jnp.cos(degree[None, :] * jnp.arccos(coords[0])[:, None])
    cheb_second = jnp.cos(degree[None, :] * jnp.arccos(coords[1])[:, None])
    real_part = charge[0][:, None] * cheb_first - charge[1][:, None] * cheb_second
    imag_part = charge[0][:, None] * cheb_second + charge[1][:, None] * cheb_first
    return jnp.concatenate([real_part, imag_part], axis=1)


def merge_children(children, operators):
    row_count, col_count, coeff_width = children.shape
    grouped = children.reshape(row_count // 2, 2, col_count // 2, 2, coeff_width)
    parent = jnp.zeros(((row_count // 2) * (col_count // 2), coeff_width), jnp.float32)
    for row_bit in range(2):
        for col_bit in range(2):
            quarter = grouped[:, row_bit, :, col_bit, :].reshape(-1, coeff_width)
            parent = parent + jnp.dot(quarter, operators[2 * row_bit + col_bit], precision=HIGHEST, preferred_element_type=jnp.float32)
    return parent.reshape(row_count // 2, col_count // 2, coeff_width)


def transfer(padded, diagonal, row_start, col_start, row_count, col_count):
    half_width = diagonal.shape[1] // 2
    row_parity = (row_start + jnp.arange(row_count, dtype=jnp.int32)) % 2
    col_parity = (col_start + jnp.arange(col_count, dtype=jnp.int32)) % 2
    summed = jnp.zeros((row_count, col_count, diagonal.shape[1]), jnp.float32)
    for shift_row in range(-3, 4):
        for shift_col in range(-3, 4):
            if max(abs(shift_row), abs(shift_col)) < 2:
                continue
            row_ok = ((shift_row >= -2 - row_parity) & (shift_row <= 3 - row_parity)).astype(jnp.float32)
            col_ok = ((shift_col >= -2 - col_parity) & (shift_col <= 3 - col_parity)).astype(jnp.float32)
            allowed = row_ok[:, None] * col_ok[None, :]
            source = padded[3 + shift_row:3 + shift_row + row_count, 3 + shift_col:3 + shift_col + col_count, :]
            factor = diagonal[(shift_row + 3) * 7 + shift_col + 3]
            diag_real = factor[:half_width]
            diag_imag = factor[half_width:]
            src_real = source[..., :half_width]
            src_imag = source[..., half_width:]
            product = jnp.concatenate([diag_real * src_real - diag_imag * src_imag, diag_real * src_imag + diag_imag * src_real], axis=-1)
            summed = summed + allowed[:, :, None] * product
    return summed


def pad_grid(current):
    return jnp.pad(current, ((3, 3), (3, 3), (0, 0)))


def whole_transfer(current, diagonal):
    return transfer(pad_grid(current), diagonal, 0, 0, current.shape[0], current.shape[1])


def reference(offsets, strengths, leaf_map, shift_matrices, transfer_diagonal):
    grid_rows = N_WIDE * LEAF_SIDE
    grid_cols = N_NARROW * LEAF_SIDE
    wide_id = lax.broadcasted_iota(jnp.int32, leaf_map.shape, 0)
    narrow_id = lax.broadcasted_iota(jnp.int32, leaf_map.shape, 1)
    global_row = wide_id * LEAF_SIDE + leaf_map // LEAF_SIDE
    global_col = narrow_id * LEAF_SIDE + leaf_map % LEAF_SIDE
    segment = (global_row * grid_cols + global_col).reshape(-1).astype(jnp.int32)
    flat_coords = offsets.reshape(2, -1)
    flat_charge = strengths.reshape(2, -1)
    panel_total = flat_coords.shape[1]
    block_size = math.gcd(panel_total, 131072)
    block_count = panel_total // block_size

    def add_block(totals, number):
        begin = (number * block_size).astype(jnp.int32)
        coords = lax.dynamic_slice_in_dim(flat_coords, begin, block_size, 1)
        charge = lax.dynamic_slice_in_dim(flat_charge, begin, block_size, 1)
        pieces = lax.dynamic_slice_in_dim(segment, begin, block_size, 0)
        return totals + jax.ops.segment_sum(panel_terms(coords, charge), pieces, num_segments=grid_rows * grid_cols), None

    totals, _ = lax.scan(add_block, jnp.zeros((grid_rows * grid_cols, 2 * ORDER), jnp.float32), jnp.arange(block_count, dtype=jnp.int32))
    leaf_grid = totals.reshape(grid_rows, grid_cols, 2 * ORDER)
    levels = {LOCAL: leaf_grid}
    for level in range(LOCAL - 1, -1, -1):
        levels[level] = merge_children(levels[level + 1], shift_matrices[COARSE + level])
    coarse_grid = merge_children(levels[0], shift_matrices[1])
    top_grid = merge_children(coarse_grid, shift_matrices[0])
    coarse_local = whole_transfer(coarse_grid, transfer_diagonal[0])
    local_zero = whole_transfer(levels[0], transfer_diagonal[1])
    local_one = whole_transfer(levels[1], transfer_diagonal[2])
    local_two = whole_transfer(levels[2], transfer_diagonal[3])
    local_three = whole_transfer(levels[3], transfer_diagonal[4])
    return (leaf_grid, local_zero, local_one, local_two, local_three, coarse_local, top_grid)
```

```python
import functools

import jax
import jax.numpy as jnp
from jax import lax
from jax.experimental import pallas as pl
from jax.experimental.pallas import tpu as pltpu
from jax.sharding import PartitionSpec as P

LANES = 128
GROUPS = 64
LEAVES = 1024
ALL = ("wide", "narrow")
F32 = jnp.float32
BF16 = jnp.bfloat16
VMEM = pl.BlockSpec(memory_space=pltpu.VMEM)
ANY = pl.BlockSpec(memory_space=pl.ANY)
HALO_ROWS = 28
HALO_COLS = 52


def split_weights(src, dst):
    for quarter in range(4):
        rows = slice(quarter * 128, (quarter + 1) * 128)
        w = src[quarter]
        high = w.astype(BF16)
        dst[rows, 0:128] = high
        dst[rows, 128:256] = (w - high.astype(F32)).astype(BF16)


def merge(x, weights):
    count = x.shape[0]
    high = x.astype(BF16).astype(F32)
    both = jnp.concatenate([high, x - high], axis=0).astype(BF16)
    y = jnp.dot(both, weights, preferred_element_type=F32)
    return y[:count, :128] + y[:count, 128:] + y[count:, :128] + y[count:, 128:]


def gather_children(src, dst, rows, cols):
    for row_bit in range(2):
        for col_bit in range(2):
            quarter = 2 * row_bit + col_bit
            lanes = slice(quarter * 128, (quarter + 1) * 128)
            for r in range(rows):
                start = (2 * r + row_bit) * 2 * cols + col_bit
                if cols > 1:
                    piece = src[pl.ds(start, cols, stride=2), :]
                else:
                    piece = src[start : start + 1, :]
                dst[r * cols : (r + 1) * cols, lanes] = piece


def up_kernel(
    off, strg, lmap, shifts,
    leaf_out, l3_out, l2_out, l1_out, l0_out, up_out, down_out,
    cheb, back, terms, acc, leaf, w_raw, w_two, x4, l4, x3, x2, x1, x0, w_sem, o_sem,
):
    w_copy = pltpu.make_async_copy(shifts.at[pl.ds(2, 5)], w_raw, w_sem)
    w_copy.start()

    for i in range(2):
        a = off[i]
        t = [None] * 9
        t[0] = jnp.ones_like(a)
        t[1] = a
        t[2] = 2.0 * a * a - 1.0
        t[3] = 2.0 * t[2] * a - a
        t[4] = 2.0 * t[2] * t[2] - 1.0
        t[5] = 2.0 * t[3] * t[2] - a
        t[6] = 2.0 * t[3] * t[3] - 1.0
        t[7] = 2.0 * t[4] * t[3] - a
        t[8] = 2.0 * t[4] * t[4] - 1.0
        for j in range(9):
            cheb[i, j * GROUPS : (j + 1) * GROUPS, :] = t[j]
        for j in range(8):
            back[i, j * GROUPS : (j + 1) * GROUPS, :] = t[8 - j]

    def make_terms(g, carry):
        blocks = []
        for i in range(2):
            now = cheb[i, pl.ds(g, 8, stride=GROUPS), :]
            before = back[i, pl.ds(g, 8, stride=GROUPS), :]
            twice = 2.0 * jnp.broadcast_to(cheb[i, pl.ds(8 * GROUPS + g, 1), :], (8, LANES))
            seq = [now]
            for _ in range(7):
                now, before = twice * now - before, now
                seq.append(now)
            blocks.append(seq)
        qr = jnp.broadcast_to(strg[0, pl.ds(g, 1), :], (8, LANES))
        qi = jnp.broadcast_to(strg[1, pl.ds(g, 1), :], (8, LANES))
        real = jnp.concatenate([qr * ca - qi * cb for ca, cb in zip(*blocks)], axis=0)
        imag = jnp.concatenate([qr * cb + qi * ca for ca, cb in zip(*blocks)], axis=0)
        whole = jnp.concatenate([real, imag], axis=0)
        high = whole.astype(BF16)
        terms[g, 0:128, :] = high
        terms[g, 128:256, :] = (whole - high.astype(F32)).astype(BF16)
        return carry

    lax.fori_loop(0, GROUPS, make_terms, 0)

    acc[...] = jnp.zeros_like(acc)
    ids = lax.broadcasted_iota(jnp.int32, (256, LANES), 0).astype(F32).astype(BF16)
    one = jnp.ones((256, LANES), BF16)
    zero = jnp.zeros((256, LANES), BF16)

    def add_chunk(k, carry):
        lefts, rights = [], []
        for j in range(8):
            g = k * 8 + j
            row = lmap[pl.ds(g, 1), :]
            parts = []
            for b in range(4):
                near = (row - 256 * b).astype(F32)
                near = jnp.broadcast_to(near, (256, LANES)).astype(BF16)
                parts.append(jnp.where(near == ids, one, zero))
            lefts.append(jnp.concatenate(parts, axis=0))
            rights.append(terms[g])
        left = jnp.concatenate(lefts, axis=1)
        right = jnp.concatenate(rights, axis=1)
        acc[...] += lax.dot_general(
            left, right, (((1,), (1,)), ((), ())), preferred_element_type=F32
        )
        return carry

    lax.fori_loop(0, GROUPS // 8, add_chunk, 0)

    leaf[...] = acc[:, 0:128] + acc[:, 128:256]
    out_copy = pltpu.make_async_copy(leaf, leaf_out, o_sem)
    out_copy.start()
    w_copy.wait()
    for t in range(5):
        split_weights(w_raw.at[t], w_two.at[t])

    gather_children(leaf, x4, 16, 16)
    l4[...] = merge(x4[...], w_two[4])
    gather_children(l4, x3, 8, 8)
    l3_out[...] = merge(x3[...], w_two[3])
    gather_children(l3_out, x2, 4, 4)
    l2_out[...] = merge(x2[...], w_two[2])
    gather_children(l2_out, x1, 2, 2)
    l1_out[...] = merge(x1[...], w_two[1])
    gather_children(l1_out, x0, 1, 1)
    l0_out[...] = jnp.broadcast_to(merge(x0[...], w_two[0])[0:1], (128, LANES))

    up_out[0:16, :] = l3_out[0:16, :]
    up_out[16:24, :] = l2_out[0:8, :]
    up_out[24:28, :] = l1_out[0:4, :]
    down_out[0:16, :] = l3_out[48:64, :]
    down_out[16:24, :] = l2_out[8:16, :]
    down_out[24:28, :] = l1_out[0:4, :]
    out_copy.wait()


def upward(offsets, strengths, leaf_map, shift_matrices):
    shape = lambda *dims: jax.ShapeDtypeStruct(dims, F32)
    scratch = lambda dims, kind=F32: pltpu.VMEM(dims, kind)
    return pl.pallas_call(
        up_kernel,
        out_shape=(
            shape(LEAVES, 128), shape(64, 128), shape(16, 128), shape(8, 128), shape(128, 128),
            shape(HALO_ROWS, 128), shape(HALO_ROWS, 128),
        ),
        in_specs=[VMEM, VMEM, VMEM, ANY],
        out_specs=(ANY,) + (VMEM,) * 6,
        scratch_shapes=[
            scratch((2, 9 * GROUPS, LANES)),
            scratch((2, 8 * GROUPS, LANES)),
            scratch((GROUPS, 256, LANES), BF16),
            scratch((LEAVES, 256)),
            scratch((LEAVES, 128)),
            scratch((5, 4, 128, 128)),
            scratch((5, 512, 256), BF16),
            scratch((256, 512)),
            scratch((256, 128)),
            scratch((64, 512)),
            scratch((16, 512)),
            scratch((8, 512)),
            scratch((8, 512)),
            pltpu.SemaphoreType.DMA,
            pltpu.SemaphoreType.DMA,
        ],
        name="upward",
    )(offsets, strengths, leaf_map, shift_matrices)


LEVELS = ((8, 0, 0), (4, 16, 24), (2, 24, 40))


def pack_kernel(l3, l2, l1, top, bottom, west_out, east_out):
    for grid, (side, row_at, col_at) in zip((l3, l2, l1), LEVELS):
        for out, first in ((west_out, 0), (east_out, side - 2)):
            for k in range(2):
                at = col_at + k * (side + 4)
                c = first + k
                out[at : at + 2, :] = top[pl.ds(row_at + c, 2, stride=side), :]
                out[at + 2 : at + 2 + side, :] = grid[pl.ds(c, side, stride=side), :]
                out[at + 2 + side : at + 4 + side, :] = bottom[pl.ds(row_at + c, 2, stride=side), :]


def pack(l3, l2, l1, top, bottom):
    return pl.pallas_call(
        pack_kernel,
        out_shape=(jax.ShapeDtypeStruct((HALO_COLS, 128), F32),) * 2,
        in_specs=[VMEM] * 5,
        out_specs=(VMEM,) * 2,
        name="pack",
    )(l3, l2, l1, top, bottom)


PITCH = 16


def make_factors(diag, same, cross):
    lane = lax.broadcasted_iota(jnp.int32, (8, LANES), 1)
    for at in (0, 8, 16, 24, 32, 40, 41):
        rows = diag[at : at + 8, :]
        turned = pltpu.roll(rows, 64, 1)
        same[at : at + 8, :] = jnp.where(lane < 64, rows, turned)
        cross[at : at + 8, :] = jnp.where(lane < 64, turned, -rows)


def transfer_rows(region, diag, same, cross, side, cols, store):
    make_factors(diag, same, cross)
    odd = (lax.broadcasted_iota(jnp.int32, (8, LANES), 0) % 2) == 1

    def factor(table, dr, dc):
        at = (dr + 3) * 7 + 3
        if dc < 3:
            return jnp.broadcast_to(table[at + dc : at + dc + 1, :], (8, LANES))
        right = jnp.broadcast_to(table[at + 3 : at + 4, :], (8, LANES))
        left = jnp.broadcast_to(table[at - 3 : at - 2, :], (8, LANES))
        return jnp.where(odd, left, right)

    def source(row, dc):
        base = row * PITCH + 4
        if dc < 3:
            return region[base + dc : base + dc + 8, :]
        return jnp.where(odd, region[base - 3 : base + 5, :], region[base + 3 : base + 11, :])

    for r in range(side):
        first = jnp.zeros((8, LANES), F32)
        second = jnp.zeros((8, LANES), F32)
        for dr in range(-2 - r % 2, 4 - r % 2):
            for dc in (-2, -1, 0, 1, 2, 3):
                if max(abs(dr), abs(dc)) < 2:
                    continue
                s = source(r + dr + 2, dc)
                first = first + factor(same, dr, dc) * s
                second = second + factor(cross, dr, dc) * s
        store(r, (first + pltpu.roll(second, 64, 1))[0:cols])


def near_kernel(
    l3, l2, l1, top, bottom, west, east, diag,
    out3, out2, out1,
    r3, r2, r1, same, cross,
):
    for grid, region, (side, row_at, col_at) in zip((l3, l2, l1), (r3, r2, r1), LEVELS):
        for r in range(side):
            at = (r + 2) * PITCH + 4
            region[at : at + side, :] = grid[r * side : (r + 1) * side, :]
        for r in range(2):
            at = r * PITCH + 4
            region[at : at + side, :] = top[row_at + r * side : row_at + (r + 1) * side, :]
            at = (r + 2 + side) * PITCH + 4
            region[at : at + side, :] = bottom[row_at + r * side : row_at + (r + 1) * side, :]
        rows = side + 4
        for k in range(2):
            at = col_at + k * rows
            region[pl.ds(2 + k, rows, stride=PITCH), :] = west[at : at + rows, :]
            region[pl.ds(4 + side + k, rows, stride=PITCH), :] = east[at : at + rows, :]
    for level, region, side, out in ((4, r3, 8, out3), (3, r2, 4, out2), (2, r1, 2, out1)):
        def store(r, value, out=out):
            out[r] = value
        transfer_rows(
            region, diag.at[level], same.at[level - 2], cross.at[level - 2], side, side, store
        )


def near(l3, l2, l1, top, bottom, west, east, diag):
    shape = lambda *dims: jax.ShapeDtypeStruct(dims, F32)
    return pl.pallas_call(
        near_kernel,
        out_shape=(shape(8, 8, 128), shape(4, 4, 128), shape(2, 2, 128)),
        in_specs=[VMEM] * 8,
        out_specs=(VMEM,) * 3,
        scratch_shapes=[
            pltpu.VMEM((12 * PITCH, 128), F32),
            pltpu.VMEM((8 * PITCH, 128), F32),
            pltpu.VMEM((6 * PITCH, 128), F32),
            pltpu.VMEM((3, 56, 128), F32),
            pltpu.VMEM((3, 56, 128), F32),
        ],
        name="near",
    )(l3, l2, l1, top, bottom, west, east, diag)


def coarse_kernel(
    roots, shifts, diag,
    out0, outc, outt,
    grid, region, w_two, xc, xt, coarse, same, cross,
):
    wide_at = lax.axis_index("wide")
    narrow_at = lax.axis_index("narrow")
    grid[...] = jnp.zeros_like(grid)
    for r in range(16):
        at = (r + 3) * PITCH + 3
        grid[at : at + 8, :] = roots[r * 8 : (r + 1) * 8, :]
    for t in range(2):
        split_weights(shifts.at[t], w_two.at[t])

    gather_children(roots, xc, 8, 4)
    coarse[...] = merge(xc[...], w_two[1])
    gather_children(coarse, xt, 4, 2)
    top = merge(xt[...], w_two[0])
    for r in range(4):
        outt[r] = top[2 * r : 2 * r + 2]

    region[...] = jnp.zeros_like(region)
    for r in range(8):
        at = (r + 2) * PITCH + 4
        region[at : at + 4, :] = coarse[4 * r : 4 * r + 4, :]
    def store(r, value):
        outc[r] = value
    transfer_rows(region, diag.at[0], same.at[0], cross.at[0], 8, 4, store)

    make_factors(diag.at[1], same.at[1], cross.at[1])
    dc = lax.broadcasted_iota(jnp.int32, (8, LANES), 0) - 3
    col_ok = (dc >= -2 - narrow_at % 2) & (dc <= 3 - narrow_at % 2)
    far = (dc >= 2) | (dc <= -2)
    first = jnp.zeros((8, LANES), F32)
    second = jnp.zeros((8, LANES), F32)
    for dr in range(-3, 4):
        row_ok = (dr >= -2 - wide_at % 2) & (dr <= 3 - wide_at % 2)
        allowed = col_ok & row_ok
        if abs(dr) < 2:
            allowed = allowed & far
        s = grid[pl.ds((wide_at + dr + 3) * PITCH + narrow_at, 8), :]
        at = (dr + 3) * 7
        first = first + jnp.where(allowed, same[1, at : at + 8, :] * s, 0.0)
        second = second + jnp.where(allowed, cross[1, at : at + 8, :] * s, 0.0)
    total = first + pltpu.roll(second, 64, 1)
    out0[0] = jnp.sum(total, axis=0, keepdims=True)


def coarse_levels(roots, shifts, diag):
    shape = lambda *dims: jax.ShapeDtypeStruct(dims, F32)
    return pl.pallas_call(
        coarse_kernel,
        out_shape=(shape(1, 1, 128), shape(8, 4, 128), shape(4, 2, 128)),
        in_specs=[
            VMEM,
            pl.BlockSpec((2, 4, 128, 128), lambda i: (0, 0, 0, 0)),
            VMEM,
        ],
        out_specs=(VMEM,) * 3,
        grid=(1,),
        scratch_shapes=[
            pltpu.VMEM((22 * PITCH, 128), F32),
            pltpu.VMEM((12 * PITCH, 128), F32),
            pltpu.VMEM((2, 512, 256), BF16),
            pltpu.VMEM((32, 512), F32),
            pltpu.VMEM((8, 512), F32),
            pltpu.VMEM((32, 128), F32),
            pltpu.VMEM((2, 56, 128), F32),
            pltpu.VMEM((2, 56, 128), F32),
        ],
        name="coarse",
    )(roots, shifts, diag)


def shift_by(x, axis, step):
    count = lax.axis_size(axis)
    pairs = [(i, i + step) for i in range(count) if 0 <= i + step < count]
    return lax.ppermute(x, axis, pairs)


def local(offsets, strengths, leaf_map, shift_matrices, transfer_diagonal):
    leaf, l3, l2, l1, l0, up, down = upward(
        offsets.reshape(2, GROUPS, LANES),
        strengths.reshape(2, GROUPS, LANES),
        leaf_map.reshape(GROUPS, LANES),
        shift_matrices,
    )
    roots = lax.all_to_all(l0, ALL, 0, 0, tiled=True)
    top = shift_by(down, "wide", 1)
    bottom = shift_by(up, "wide", -1)
    to_west, to_east = pack(l3, l2, l1, top, bottom)
    west = shift_by(to_east, "narrow", 1)
    east = shift_by(to_west, "narrow", -1)
    local_three, local_two, local_one = near(l3, l2, l1, top, bottom, west, east, transfer_diagonal)
    local_zero, coarse_local, top_grid = coarse_levels(roots, shift_matrices, transfer_diagonal)
    return (
        leaf.reshape(32, 32, 128), local_zero, local_one, local_two, local_three,
        coarse_local, top_grid,
    )


def solution(mesh):
    return jax.shard_map(
        local,
        mesh=mesh,
        in_specs=(
            P(None, "wide", "narrow", None),
            P(None, "wide", "narrow", None),
            P("wide", "narrow", None),
            P(),
            P(),
        ),
        out_specs=(
            P("wide", "narrow", None),
            P("wide", "narrow", None),
            P("wide", "narrow", None),
            P("wide", "narrow", None),
            P("wide", "narrow", None),
            P(),
            P(),
        ),
        check_vma=False,
    )
```

```python
import functools

import jax
import jax.numpy as jnp
from jax import lax
from jax.experimental import pallas as pl
from jax.experimental.pallas import tpu as pltpu
from jax.sharding import PartitionSpec as P

LANES = 128
GROUPS = 64
STEP = 16
LEAVES = 1024
ALL = ("wide", "narrow")
F32 = jnp.float32
BF16 = jnp.bfloat16
VMEM = pl.BlockSpec(memory_space=pltpu.VMEM)
ANY = pl.BlockSpec(memory_space=pl.ANY)
HALO_ROWS = 28
HALO_COLS = 52
CHUNK_WIDE = 32
CHUNK_NARROW = 72


def near_memory(*dims, kind=F32):
    return pltpu.VMEM(dims, kind)


def kept_near(*arrays):
    return tuple(pltpu.with_memory_space_constraint(a, pltpu.VMEM) for a in arrays)


PARTS = 4


def write_leaves(leaf, leaf_out, sem):
    rows = LEAVES // PARTS
    copies = [
        pltpu.make_async_copy(leaf.at[pl.ds(i * rows, rows)], leaf_out.at[pl.ds(i * rows, rows)], sem.at[i])
        for i in range(PARTS)
    ]
    for copy in copies:
        copy.start()
    return copies


def split_weights(src, dst):
    for quarter in range(4):
        rows = slice(quarter * 128, (quarter + 1) * 128)
        w = src[quarter]
        high = w.astype(BF16)
        dst[rows, 0:128] = high
        dst[rows, 128:256] = (w - high.astype(F32)).astype(BF16)


def merge(x, weights):
    count = x.shape[0]
    high = x.astype(BF16).astype(F32)
    both = jnp.concatenate([high, x - high], axis=0).astype(BF16)
    y = jnp.dot(both, weights, preferred_element_type=F32)
    return y[:count, :128] + y[:count, 128:] + y[count:, :128] + y[count:, 128:]


def gather_children(src, dst, rows, cols):
    for row_bit in range(2):
        for col_bit in range(2):
            quarter = 2 * row_bit + col_bit
            lanes = slice(quarter * 128, (quarter + 1) * 128)
            for r in range(rows):
                start = (2 * r + row_bit) * 2 * cols + col_bit
                if cols > 1:
                    piece = src[pl.ds(start, cols, stride=2), :]
                else:
                    piece = src[start : start + 1, :]
                dst[r * cols : (r + 1) * cols, lanes] = piece


def make_factors(diag, same, cross):
    lane = lax.broadcasted_iota(jnp.int32, (8, LANES), 1)
    for at in (0, 8, 16, 24, 32, 40, 41):
        rows = diag[at : at + 8, :]
        turned = pltpu.roll(rows, 64, 1)
        same[at : at + 8, :] = jnp.where(lane < 64, rows, turned)
        cross[at : at + 8, :] = jnp.where(lane < 64, turned, -rows)


def up_kernel(
    off, strg, lmap, diag, shifts,
    leaf, l3_out, l2_out, l1_out, send_out, w_low, same, cross,
    cheb, back, even, odd, acc, w_raw, w_two, x4, l4, x3, x2, x1, x0, w_sem,
):
    w_copy = pltpu.make_async_copy(shifts, w_raw, w_sem)
    w_copy.start()

    for i in range(2):
        a = off[i]
        t = [None] * 9
        t[0] = jnp.ones_like(a)
        t[1] = a
        t[2] = 2.0 * a * a - 1.0
        t[3] = 2.0 * t[2] * a - a
        t[4] = 2.0 * t[2] * t[2] - 1.0
        t[5] = 2.0 * t[3] * t[2] - a
        t[6] = 2.0 * t[3] * t[3] - 1.0
        t[7] = 2.0 * t[4] * t[3] - a
        t[8] = 2.0 * t[4] * t[4] - 1.0
        for j in range(9):
            cheb[i, j * GROUPS : (j + 1) * GROUPS, :] = t[j]
        for j in range(8):
            back[i, j * GROUPS : (j + 1) * GROUPS, :] = t[8 - j]

    def make_terms(g, out, j):
        blocks = []
        for i in range(2):
            now = cheb[i, pl.ds(g, 8, stride=GROUPS), :]
            before = back[i, pl.ds(g, 8, stride=GROUPS), :]
            twice = 2.0 * jnp.broadcast_to(cheb[i, pl.ds(8 * GROUPS + g, 1), :], (8, LANES))
            seq = [now]
            for _ in range(7):
                now, before = twice * now - before, now
                seq.append(now)
            blocks.append(seq)
        qr = jnp.broadcast_to(strg[0, pl.ds(g, 1), :], (8, LANES))
        qi = jnp.broadcast_to(strg[1, pl.ds(g, 1), :], (8, LANES))
        real = jnp.concatenate([qr * ca - qi * cb for ca, cb in zip(*blocks)], axis=0)
        imag = jnp.concatenate([qr * cb + qi * ca for ca, cb in zip(*blocks)], axis=0)
        whole = jnp.concatenate([real, imag], axis=0)
        high = whole.astype(BF16)
        lanes = slice(j * LANES, (j + 1) * LANES)
        out[0:128, lanes] = high
        out[128:256, lanes] = (whole - high.astype(F32)).astype(BF16)

    ids = lax.broadcasted_iota(jnp.int32, (256, LANES), 0).astype(F32).astype(BF16)
    one = jnp.ones((256, LANES), BF16)
    zero = jnp.zeros((256, LANES), BF16)

    def terms_of(k, out):
        for j in range(STEP):
            make_terms(k * STEP + j, out, j)

    def add_chunk(k, right):
        lefts = []
        for j in range(STEP):
            row = lmap[pl.ds(k * STEP + j, 1), :]
            parts = []
            for b in range(4):
                near = (row - 256 * b).astype(F32)
                near = jnp.broadcast_to(near, (256, LANES)).astype(BF16)
                parts.append(jnp.where(near == ids, one, zero))
            lefts.append(jnp.concatenate(parts, axis=0))
        left = jnp.concatenate(lefts, axis=1)
        return lax.dot_general(
            left, right[...], (((1,), (1,)), ((), ())), preferred_element_type=F32
        )

    terms_of(0, even)
    terms_of(1, odd)
    acc[...] = add_chunk(0, even)
    terms_of(2, even)
    acc[...] += add_chunk(1, odd)
    terms_of(3, odd)
    acc[...] += add_chunk(2, even)
    whole = acc[...] + add_chunk(3, odd)
    leaf[...] = whole[:, 0:128] + whole[:, 128:256]

    w_copy.wait()
    for t in range(2):
        split_weights(w_raw.at[t], w_low.at[t])
    for t in range(2, 7):
        split_weights(w_raw.at[t], w_two.at[t - 2])
    for level in range(5):
        make_factors(diag.at[level], same.at[level], cross.at[level])
    gather_children(leaf, x4, 16, 16)
    l4[...] = merge(x4[...], w_two[4])
    gather_children(l4, x3, 8, 8)
    l3_out[...] = merge(x3[...], w_two[3])
    gather_children(l3_out, x2, 4, 4)
    l2_out[...] = merge(x2[...], w_two[2])
    gather_children(l2_out, x1, 2, 2)
    l1_out[...] = merge(x1[...], w_two[1])
    gather_children(l1_out, x0, 1, 1)
    root = merge(x0[...], w_two[0])[0:1]
    send_out[pl.ds(HALO_ROWS, 16, stride=CHUNK_WIDE), :] = jnp.broadcast_to(root, (16, LANES))

    wide_at = lax.axis_index("wide")

    def put(chunk, l3_row, l2_row):
        at = pl.multiple_of(chunk * CHUNK_WIDE, 8)
        send_out[pl.ds(at, 16), :] = l3_out[l3_row : l3_row + 16, :]
        send_out[pl.ds(at + 16, 8), :] = l2_out[l2_row : l2_row + 8, :]
        send_out[pl.ds(at + 24, 4), :] = l1_out[0:4, :]

    @pl.when(wide_at > 0)
    def _():
        put(wide_at - 1, 0, 0)

    @pl.when(wide_at < 15)
    def _():
        put(wide_at + 1, 48, 8)


def upward(*operands):
    scratch = lambda dims, kind=F32: pltpu.VMEM(dims, kind)
    return pl.pallas_call(
        up_kernel,
        out_shape=(
            near_memory(LEAVES, 128), near_memory(64, 128), near_memory(16, 128),
            near_memory(8, 128), near_memory(16 * CHUNK_WIDE, 128),
            near_memory(2, 512, 256, kind=BF16), near_memory(5, 56, 128), near_memory(5, 56, 128),
        ),
        in_specs=[VMEM, VMEM, VMEM, VMEM, ANY],
        out_specs=(VMEM,) * 8,
        scratch_shapes=[
            scratch((2, 9 * GROUPS, LANES)),
            scratch((2, 8 * GROUPS, LANES)),
            scratch((256, STEP * LANES), BF16),
            scratch((256, STEP * LANES), BF16),
            scratch((LEAVES, 256)),
            scratch((7, 4, 128, 128)),
            scratch((5, 512, 256), BF16),
            scratch((256, 512)),
            scratch((256, 128)),
            scratch((64, 512)),
            scratch((16, 512)),
            scratch((8, 512)),
            scratch((8, 512)),
            pltpu.SemaphoreType.DMA,
        ],
        name="upward",
    )(*operands)


LEVELS = ((8, 0, 0), (4, 16, 24), (2, 24, 40))


def edge_rows(got, wide_at, top, bottom):
    above = pl.multiple_of(jnp.maximum(wide_at - 1, 0) * CHUNK_WIDE, 8)
    below = pl.multiple_of(jnp.minimum(wide_at + 1, 15) * CHUNK_WIDE, 8)
    top[...] = jnp.where(wide_at > 0, got[pl.ds(above, 32), :], 0.0)
    bottom[...] = jnp.where(wide_at < 15, got[pl.ds(below, 32), :], 0.0)


def pack_kernel(l3, l2, l1, got, send_out, top, bottom):
    wide_at = lax.axis_index("wide")
    narrow_at = lax.axis_index("narrow")
    edge_rows(got, wide_at, top, bottom)
    roots = got[pl.ds(HALO_ROWS, 16, stride=CHUNK_WIDE), :]
    for j in range(8):
        at = j * CHUNK_NARROW + HALO_COLS
        send_out[at : at + 16, :] = roots

    def put(chunk, first_of):
        base = pl.multiple_of(chunk * CHUNK_NARROW, 8)
        for grid, (side, row_at, col_at) in zip((l3, l2, l1), LEVELS):
            for k in range(2):
                at = base + col_at + k * (side + 4)
                c = first_of(side) + k
                send_out[pl.ds(at, 2), :] = top[pl.ds(row_at + c, 2, stride=side), :]
                send_out[pl.ds(at + 2, side), :] = grid[pl.ds(c, side, stride=side), :]
                send_out[pl.ds(at + 2 + side, 2), :] = bottom[pl.ds(row_at + c, 2, stride=side), :]

    @pl.when(narrow_at > 0)
    def _():
        put(narrow_at - 1, lambda side: 0)

    @pl.when(narrow_at < 7)
    def _():
        put(narrow_at + 1, lambda side: side - 2)


def pack(l3, l2, l1, got):
    return pl.pallas_call(
        pack_kernel,
        out_shape=(
            near_memory(8 * CHUNK_NARROW, 128), near_memory(32, 128), near_memory(32, 128),
        ),
        in_specs=[VMEM] * 4,
        out_specs=(VMEM,) * 3,
        name="pack",
    )(l3, l2, l1, got)


PITCH = 16


def transfer_rows(region, same, cross, side, cols, store):
    odd = (lax.broadcasted_iota(jnp.int32, (8, LANES), 0) % 2) == 1

    def factor(table, dr, dc):
        at = (dr + 3) * 7 + 3
        if dc < 3:
            return jnp.broadcast_to(table[at + dc : at + dc + 1, :], (8, LANES))
        right = jnp.broadcast_to(table[at + 3 : at + 4, :], (8, LANES))
        left = jnp.broadcast_to(table[at - 3 : at - 2, :], (8, LANES))
        return jnp.where(odd, left, right)

    def source(row, dc):
        base = row * PITCH + 4
        if dc < 3:
            return region[base + dc : base + dc + 8, :]
        return jnp.where(odd, region[base - 3 : base + 5, :], region[base + 3 : base + 11, :])

    for r in range(side):
        first = jnp.zeros((8, LANES), F32)
        second = jnp.zeros((8, LANES), F32)
        for dr in range(-2 - r % 2, 4 - r % 2):
            for dc in (-2, -1, 0, 1, 2, 3):
                if max(abs(dr), abs(dc)) < 2:
                    continue
                s = source(r + dr + 2, dc)
                first = first + factor(same, dr, dc) * s
                second = second + factor(cross, dr, dc) * s
        store(r, (first + pltpu.roll(second, 64, 1))[0:cols])


def down_kernel(
    l3, l2, l1, leaf, top, bottom, got_cols, w_two, same, cross,
    leaf_out, out0, out1, out2, out3, outc, outt,
    r3, r2, r1, west, east, grid, region, xc, xt, coarse, sem,
):
    copies = write_leaves(leaf, leaf_out, sem)
    wide_at = lax.axis_index("wide")
    narrow_at = lax.axis_index("narrow")
    before = pl.multiple_of(jnp.maximum(narrow_at - 1, 0) * CHUNK_NARROW, 8)
    after = pl.multiple_of(jnp.minimum(narrow_at + 1, 7) * CHUNK_NARROW, 8)
    west[...] = jnp.where(narrow_at > 0, got_cols[pl.ds(before, 56), :], 0.0)
    east[...] = jnp.where(narrow_at < 7, got_cols[pl.ds(after, 56), :], 0.0)

    grid[...] = jnp.zeros_like(grid)
    for j in range(8):
        at = j * CHUNK_NARROW + HALO_COLS
        grid[pl.ds(3 * PITCH + 3 + j, 16, stride=PITCH), :] = got_cols[at : at + 16, :]
    for row_bit in range(2):
        for col_bit in range(2):
            lanes = slice((2 * row_bit + col_bit) * 128, (2 * row_bit + col_bit + 1) * 128)
            for r in range(8):
                at = (2 * r + row_bit + 3) * PITCH + 3 + col_bit
                xc[4 * r : 4 * r + 4, lanes] = grid[pl.ds(at, 4, stride=2), :]
    coarse[...] = merge(xc[...], w_two[1])
    gather_children(coarse, xt, 4, 2)
    peak = merge(xt[...], w_two[0])
    for r in range(4):
        outt[r] = peak[2 * r : 2 * r + 2]

    for level, region_k, (side, row_at, col_at) in zip((l3, l2, l1), (r3, r2, r1), LEVELS):
        for r in range(side):
            at = (r + 2) * PITCH + 4
            region_k[at : at + side, :] = level[r * side : (r + 1) * side, :]
        for r in range(2):
            at = r * PITCH + 4
            region_k[at : at + side, :] = top[row_at + r * side : row_at + (r + 1) * side, :]
            at = (r + 2 + side) * PITCH + 4
            region_k[at : at + side, :] = bottom[row_at + r * side : row_at + (r + 1) * side, :]
        rows = side + 4
        for k in range(2):
            at = col_at + k * rows
            region_k[pl.ds(2 + k, rows, stride=PITCH), :] = west[at : at + rows, :]
            region_k[pl.ds(4 + side + k, rows, stride=PITCH), :] = east[at : at + rows, :]
    for level, region_k, side, out in ((4, r3, 8, out3), (3, r2, 4, out2), (2, r1, 2, out1)):
        def store(r, value, out=out):
            out[r] = value
        transfer_rows(region_k, same.at[level], cross.at[level], side, side, store)

    region[...] = jnp.zeros_like(region)
    for r in range(8):
        at = (r + 2) * PITCH + 4
        region[at : at + 4, :] = coarse[4 * r : 4 * r + 4, :]

    def store_coarse(r, value):
        outc[r] = value

    transfer_rows(region, same.at[0], cross.at[0], 8, 4, store_coarse)

    dc = lax.broadcasted_iota(jnp.int32, (8, LANES), 0) - 3
    col_ok = (dc >= -2 - narrow_at % 2) & (dc <= 3 - narrow_at % 2)
    far = (dc >= 2) | (dc <= -2)
    first = jnp.zeros((8, LANES), F32)
    second = jnp.zeros((8, LANES), F32)
    for dr in range(-3, 4):
        row_ok = (dr >= -2 - wide_at % 2) & (dr <= 3 - wide_at % 2)
        allowed = col_ok & row_ok
        if abs(dr) < 2:
            allowed = allowed & far
        s = grid[pl.ds((wide_at + dr + 3) * PITCH + narrow_at, 8), :]
        at = (dr + 3) * 7
        first = first + jnp.where(allowed, same[1, at : at + 8, :] * s, 0.0)
        second = second + jnp.where(allowed, cross[1, at : at + 8, :] * s, 0.0)
    total = first + pltpu.roll(second, 64, 1)
    out0[0] = jnp.sum(total, axis=0, keepdims=True)
    for copy in copies:
        copy.wait()


def downward(*operands):
    shape = lambda *dims: jax.ShapeDtypeStruct(dims, F32)
    tall = lambda rows: pltpu.VMEM((rows, 128), F32)
    return pl.pallas_call(
        down_kernel,
        out_shape=(
            shape(LEAVES, 128),
            shape(1, 1, 128), shape(2, 2, 128), shape(4, 4, 128), shape(8, 8, 128),
            shape(8, 4, 128), shape(4, 2, 128),
        ),
        in_specs=[VMEM] * 10,
        out_specs=(ANY,) + (VMEM,) * 6,
        scratch_shapes=[
            tall(12 * PITCH), tall(8 * PITCH), tall(6 * PITCH),
            tall(56), tall(56),
            tall(22 * PITCH), tall(12 * PITCH),
            pltpu.VMEM((32, 512), F32), pltpu.VMEM((8, 512), F32), tall(32),
            pltpu.SemaphoreType.DMA((PARTS,)),
        ],
        name="downward",
    )(*operands)


def local(offsets, strengths, leaf_map, shift_matrices, transfer_diagonal):
    leaf, l3, l2, l1, send, *tables = upward(
        offsets.reshape(2, GROUPS, LANES),
        strengths.reshape(2, GROUPS, LANES),
        leaf_map.reshape(GROUPS, LANES),
        transfer_diagonal,
        shift_matrices,
    )
    got_rows = lax.all_to_all(send, "wide", 0, 0, tiled=True)
    l3, l2, l1, got_rows = kept_near(l3, l2, l1, got_rows)
    send, top, bottom = pack(l3, l2, l1, got_rows)
    got_cols = lax.all_to_all(send, "narrow", 0, 0, tiled=True)
    leaf, local_zero, local_one, local_two, local_three, coarse_local, top_grid = downward(
        l3, l2, l1, *kept_near(leaf, top, bottom, got_cols, *tables)
    )
    return (
        leaf.reshape(32, 32, 128), local_zero, local_one, local_two, local_three,
        coarse_local, top_grid,
    )


def solution(mesh):
    return jax.shard_map(
        local,
        mesh=mesh,
        in_specs=(
            P(None, "wide", "narrow", None),
            P(None, "wide", "narrow", None),
            P("wide", "narrow", None),
            P(),
            P(),
        ),
        out_specs=(
            P("wide", "narrow", None),
            P("wide", "narrow", None),
            P("wide", "narrow", None),
            P("wide", "narrow", None),
            P("wide", "narrow", None),
            P(),
            P(),
        ),
        check_vma=False,
    )
```

```python
import functools

import jax
import jax.numpy as jnp
from jax import lax
from jax.experimental import pallas as pl
from jax.experimental.pallas import tpu as pltpu
from jax.sharding import PartitionSpec as P

LANES = 128
GROUPS = 64
CHUNKS = (16, 16, 16, 16)
LEAVES = 1024
ALL = ("wide", "narrow")
F32 = jnp.float32
BF16 = jnp.bfloat16
VMEM = pl.BlockSpec(memory_space=pltpu.VMEM)
ANY = pl.BlockSpec(memory_space=pl.ANY)
HALO_ROWS = 28
CHUNK_WIDE = 29
CHUNK_NARROW = 44


def near_memory(*dims, kind=F32):
    return pltpu.VMEM(dims, kind)


def kept_near(*arrays):
    return tuple(pltpu.with_memory_space_constraint(a, pltpu.VMEM) for a in arrays)


PARTS = 4


def write_leaves(leaf, leaf_out, sem):
    rows = LEAVES // PARTS
    copies = [
        pltpu.make_async_copy(leaf.at[pl.ds(i * rows, rows)], leaf_out.at[pl.ds(i * rows, rows)], sem.at[i])
        for i in range(PARTS)
    ]
    for copy in copies:
        copy.start()
    return copies


def split_weights(src, dst):
    for quarter in range(4):
        rows = slice(quarter * 128, (quarter + 1) * 128)
        w = src[quarter]
        high = w.astype(BF16)
        dst[rows, 0:128] = high
        dst[rows, 128:256] = (w - high.astype(F32)).astype(BF16)


def merge(x, weights):
    count = x.shape[0]
    high = x.astype(BF16).astype(F32)
    both = jnp.concatenate([high, x - high], axis=0).astype(BF16)
    y = jnp.dot(both, weights, preferred_element_type=F32)
    return y[:count, :128] + y[:count, 128:] + y[count:, :128] + y[count:, 128:]


def gather_children(src, dst, rows, cols):
    for row_bit in range(2):
        for col_bit in range(2):
            quarter = 2 * row_bit + col_bit
            lanes = slice(quarter * 128, (quarter + 1) * 128)
            for r in range(rows):
                start = (2 * r + row_bit) * 2 * cols + col_bit
                if cols > 1:
                    piece = src[pl.ds(start, cols, stride=2), :]
                else:
                    piece = src[start : start + 1, :]
                dst[r * cols : (r + 1) * cols, lanes] = piece


def make_factors(diag, same, cross):
    lane = lax.broadcasted_iota(jnp.int32, (8, LANES), 1)
    for at in (0, 8, 16, 24, 32, 40, 41):
        rows = diag[at : at + 8, :]
        turned = pltpu.roll(rows, 64, 1)
        same[at : at + 8, :] = jnp.where(lane < 64, rows, turned)
        cross[at : at + 8, :] = jnp.where(lane < 64, turned, -rows)


def up_kernel(
    off, strg, lmap, diag, shifts,
    leaf_out, l3_out, l2_out, l1_out, send_out, w_low, same, cross,
    cheb, back, even, odd, acc, leaf, w_raw, w_two, x4, l4, x3, x2, x1, x0, w_sem, o_sem,
):
    w_copy = pltpu.make_async_copy(shifts, w_raw, w_sem)
    w_copy.start()

    for i in range(2):
        a = off[i]
        t = [None] * 9
        t[0] = jnp.ones_like(a)
        t[1] = a
        t[2] = 2.0 * a * a - 1.0
        t[3] = 2.0 * t[2] * a - a
        t[4] = 2.0 * t[2] * t[2] - 1.0
        t[5] = 2.0 * t[3] * t[2] - a
        t[6] = 2.0 * t[3] * t[3] - 1.0
        t[7] = 2.0 * t[4] * t[3] - a
        t[8] = 2.0 * t[4] * t[4] - 1.0
        for j in range(9):
            cheb[i, j * GROUPS : (j + 1) * GROUPS, :] = t[j]
        for j in range(8):
            back[i, j * GROUPS : (j + 1) * GROUPS, :] = t[8 - j]

    def make_terms(g, out, j):
        blocks = []
        for i in range(2):
            now = cheb[i, pl.ds(g, 8, stride=GROUPS), :]
            before = back[i, pl.ds(g, 8, stride=GROUPS), :]
            twice = 2.0 * jnp.broadcast_to(cheb[i, pl.ds(8 * GROUPS + g, 1), :], (8, LANES))
            seq = [now]
            for _ in range(7):
                now, before = twice * now - before, now
                seq.append(now)
            blocks.append(seq)
        qr = jnp.broadcast_to(strg[0, pl.ds(g, 1), :], (8, LANES))
        qi = jnp.broadcast_to(strg[1, pl.ds(g, 1), :], (8, LANES))
        real = jnp.concatenate([qr * ca - qi * cb for ca, cb in zip(*blocks)], axis=0)
        imag = jnp.concatenate([qr * cb + qi * ca for ca, cb in zip(*blocks)], axis=0)
        whole = jnp.concatenate([real, imag], axis=0)
        high = whole.astype(BF16)
        lanes = slice(j * LANES, (j + 1) * LANES)
        out[0:128, lanes] = high
        out[128:256, lanes] = (whole - high.astype(F32)).astype(BF16)

    ids = lax.broadcasted_iota(jnp.int32, (256, LANES), 0).astype(F32).astype(BF16)
    one = jnp.ones((256, LANES), BF16)
    zero = jnp.zeros((256, LANES), BF16)

    def terms_of(groups, out):
        for j, g in enumerate(groups):
            make_terms(g, out, j)

    def sums_of(groups, right):
        lefts = []
        for g in groups:
            row = lmap[pl.ds(g, 1), :]
            parts = []
            for b in range(4):
                near = (row - 256 * b).astype(F32)
                near = jnp.broadcast_to(near, (256, LANES)).astype(BF16)
                parts.append(jnp.where(near == ids, one, zero))
            lefts.append(jnp.concatenate(parts, axis=0))
        left = jnp.concatenate(lefts, axis=1)
        return lax.dot_general(
            left, right[:, 0 : len(groups) * LANES], (((1,), (1,)), ((), ())),
            preferred_element_type=F32,
        )

    chunks, at = [], 0
    for size in CHUNKS:
        chunks.append(range(at, at + size))
        at += size
    buffers = (even, odd)
    terms_of(chunks[0], even)
    for level in range(5):
        make_factors(diag.at[level], same.at[level], cross.at[level])
    for k, groups in enumerate(chunks):
        if k + 1 < len(chunks):
            terms_of(chunks[k + 1], buffers[(k + 1) % 2])
        part = sums_of(groups, buffers[k % 2])
        if k == 0:
            acc[...] = part
        elif k + 1 < len(chunks):
            acc[...] += part
        else:
            part = acc[...] + part
            leaf[...] = part[:, 0:128] + part[:, 128:256]
    copies = write_leaves(leaf, leaf_out, o_sem)
    w_copy.wait()
    for t in range(7):
        split_weights(w_raw.at[t], w_low.at[t] if t < 2 else w_two.at[t - 2])

    gather_children(leaf, x4, 16, 16)
    l4[...] = merge(x4[...], w_two[4])
    gather_children(l4, x3, 8, 8)
    l3_out[...] = merge(x3[...], w_two[3])
    gather_children(l3_out, x2, 4, 4)
    l2_out[...] = merge(x2[...], w_two[2])
    gather_children(l2_out, x1, 2, 2)
    l1_out[...] = merge(x1[...], w_two[1])
    gather_children(l1_out, x0, 1, 1)
    root = merge(x0[...], w_two[0])[0:1]
    send_out[pl.ds(HALO_ROWS, 16, stride=CHUNK_WIDE), :] = jnp.broadcast_to(root, (16, LANES))

    wide_at = lax.axis_index("wide")

    def put(chunk, l3_row, l2_row):
        at = chunk * CHUNK_WIDE
        send_out[pl.ds(at, 16), :] = l3_out[l3_row : l3_row + 16, :]
        send_out[pl.ds(at + 16, 8), :] = l2_out[l2_row : l2_row + 8, :]
        send_out[pl.ds(at + 24, 4), :] = l1_out[0:4, :]

    @pl.when(wide_at > 0)
    def _():
        put(wide_at - 1, 0, 0)

    @pl.when(wide_at < 15)
    def _():
        put(wide_at + 1, 48, 8)

    for copy in copies:
        copy.wait()


def upward(*operands):
    scratch = lambda dims, kind=F32: pltpu.VMEM(dims, kind)
    return pl.pallas_call(
        up_kernel,
        out_shape=(
            jax.ShapeDtypeStruct((LEAVES, 128), F32), near_memory(64, 128), near_memory(16, 128),
            near_memory(8, 128), near_memory(16 * CHUNK_WIDE, 128),
            near_memory(2, 512, 256, kind=BF16), near_memory(5, 56, 128), near_memory(5, 56, 128),
        ),
        in_specs=[VMEM, VMEM, VMEM, VMEM, ANY],
        out_specs=(ANY,) + (VMEM,) * 7,
        scratch_shapes=[
            scratch((2, 9 * GROUPS, LANES)),
            scratch((2, 8 * GROUPS, LANES)),
            scratch((256, max(CHUNKS) * LANES), BF16),
            scratch((256, max(CHUNKS) * LANES), BF16),
            scratch((LEAVES, 256)),
            scratch((LEAVES, 128)),
            scratch((7, 4, 128, 128)),
            scratch((5, 512, 256), BF16),
            scratch((256, 512)),
            scratch((256, 128)),
            scratch((64, 512)),
            scratch((16, 512)),
            scratch((8, 512)),
            scratch((8, 512)),
            pltpu.SemaphoreType.DMA,
            pltpu.SemaphoreType.DMA((PARTS,)),
        ],
        name="upward",
    )(*operands)


PITCH = 16
LEVELS = ((8, 0), (4, 16), (2, 24))
SAVED = (0, 64, 96)


def transfer_rows(region, same, cross, side, cols, store):
    odd = (lax.broadcasted_iota(jnp.int32, (8, LANES), 0) % 2) == 1

    def factor(table, dr, dc):
        at = (dr + 3) * 7 + 3
        if dc < 3:
            return jnp.broadcast_to(table[at + dc : at + dc + 1, :], (8, LANES))
        right = jnp.broadcast_to(table[at + 3 : at + 4, :], (8, LANES))
        left = jnp.broadcast_to(table[at - 3 : at - 2, :], (8, LANES))
        return jnp.where(odd, left, right)

    def source(row, dc):
        base = row * PITCH + 4
        if dc < 3:
            return region[base + dc : base + dc + 8, :]
        return jnp.where(odd, region[base - 3 : base + 5, :], region[base + 3 : base + 11, :])

    for r in range(side):
        first = jnp.zeros((8, LANES), F32)
        second = jnp.zeros((8, LANES), F32)
        for dr in range(-2 - r % 2, 4 - r % 2):
            for dc in (-2, -1, 0, 1, 2, 3):
                if max(abs(dr), abs(dc)) < 2:
                    continue
                s = source(r + dr + 2, dc)
                first = first + factor(same, dr, dc) * s
                second = second + factor(cross, dr, dc) * s
        store(r, (first + pltpu.roll(second, 64, 1))[0:cols])


def column_products(column, same, cross, dcs):
    odd = (lax.broadcasted_iota(jnp.int32, (8, LANES), 0) % 2) == 1
    first = jnp.zeros((8, LANES), F32)
    second = jnp.zeros((8, LANES), F32)

    def factor(table, dr, dc):
        at = (dr + 3) * 7 + dc + 3
        if dr < 3:
            return jnp.broadcast_to(table[at : at + 1, :], (8, LANES))
        low = jnp.broadcast_to(table[dc + 3 : dc + 4, :], (8, LANES))
        high = jnp.broadcast_to(table[at : at + 1, :], (8, LANES))
        return jnp.where(odd, low, high)

    for k, dc in enumerate(dcs):
        for dr in (-2, -1, 0, 1, 2, 3):
            if max(abs(dr), abs(dc)) < 2:
                continue
            at = k * PITCH + 4
            if dr < 3:
                s = column[at + dr : at + dr + 8, :]
            else:
                s = jnp.where(odd, column[at - 3 : at + 5, :], column[at + 3 : at + 11, :])
            first = first + factor(same, dr, dc) * s
            second = second + factor(cross, dr, dc) * s
    return first + pltpu.roll(second, 64, 1)


def pack_kernel(l3, l2, l1, got, same, cross, send_out, top, bottom, columns):
    wide_at = lax.axis_index("wide")
    narrow_at = lax.axis_index("narrow")
    above = jnp.maximum(wide_at - 1, 0) * CHUNK_WIDE
    below = jnp.minimum(wide_at + 1, 15) * CHUNK_WIDE
    top[0:HALO_ROWS, :] = jnp.where(wide_at > 0, got[pl.ds(above, HALO_ROWS), :], 0.0)
    bottom[0:HALO_ROWS, :] = jnp.where(wide_at < 15, got[pl.ds(below, HALO_ROWS), :], 0.0)
    roots = got[pl.ds(HALO_ROWS, 16, stride=CHUNK_WIDE), :]
    for j in range(8):
        at = j * CHUNK_NARROW + HALO_ROWS
        send_out[at : at + 16, :] = roots

    results = []
    for number, (grid, (side, row_at)) in enumerate(zip((l3, l2, l1), LEVELS)):
        level = 4 - number
        for east in range(2):
            column = columns.at[2 * number + east]
            for k in range(2):
                c = k + east * (side - 2)
                at = k * PITCH + 2
                column[at : at + 2, :] = top[pl.ds(row_at + c, 2, stride=side), :]
                column[at + 2 : at + 2 + side, :] = grid[pl.ds(c, side, stride=side), :]
                column[at + 2 + side : at + 4 + side, :] = bottom[pl.ds(row_at + c, 2, stride=side), :]
            for target, dcs in enumerate(((-2, -1), (-3, -2)) if east else ((2, 3), (1, 2))):
                value = column_products(column, same.at[level], cross.at[level], dcs)
                results.append((east, row_at + target * side, value[0:side]))

    for east in range(2):
        @pl.when((narrow_at < 7) if east else (narrow_at > 0))
        def _():
            base = (narrow_at + (1 if east else -1)) * CHUNK_NARROW
            for which, at, value in results:
                if which == east:
                    send_out[pl.ds(base + at, value.shape[0]), :] = value


def pack(*operands):
    return pl.pallas_call(
        pack_kernel,
        out_shape=(
            near_memory(8 * CHUNK_NARROW, 128), near_memory(32, 128), near_memory(32, 128),
        ),
        in_specs=[VMEM] * 6,
        out_specs=(VMEM,) * 3,
        scratch_shapes=[pltpu.VMEM((6, 2 * PITCH, 128), F32)],
        name="pack",
    )(*operands)


def down_kernel(
    l3, l2, l1, top, bottom, got, w_two, same, cross,
    out0, out1, out2, out3, outc, outt,
    r3, r2, r1, total, grid, region, xc, xt, coarse,
):
    wide_at = lax.axis_index("wide")
    narrow_at = lax.axis_index("narrow")
    grid[...] = jnp.zeros_like(grid)
    for j in range(8):
        at = j * CHUNK_NARROW + HALO_ROWS
        grid[pl.ds(3 * PITCH + 3 + j, 16, stride=PITCH), :] = got[at : at + 16, :]
    for row_bit in range(2):
        for col_bit in range(2):
            lanes = slice((2 * row_bit + col_bit) * 128, (2 * row_bit + col_bit + 1) * 128)
            for r in range(8):
                at = (2 * r + row_bit + 3) * PITCH + 3 + col_bit
                xc[4 * r : 4 * r + 4, lanes] = grid[pl.ds(at, 4, stride=2), :]
    coarse[...] = merge(xc[...], w_two[1])
    gather_children(coarse, xt, 4, 2)
    peak = merge(xt[...], w_two[0])
    for r in range(4):
        outt[r] = peak[2 * r : 2 * r + 2]

    for number, (own, region_k, (side, row_at)) in enumerate(
        zip((l3, l2, l1), (r3, r2, r1), LEVELS)
    ):
        region_k[...] = jnp.zeros_like(region_k)
        for r in range(side):
            at = (r + 2) * PITCH + 4
            region_k[at : at + side, :] = own[r * side : (r + 1) * side, :]
        for r in range(2):
            at = r * PITCH + 4
            region_k[at : at + side, :] = top[row_at + r * side : row_at + (r + 1) * side, :]
            at = (r + 2 + side) * PITCH + 4
            region_k[at : at + side, :] = bottom[row_at + r * side : row_at + (r + 1) * side, :]

        def store(r, value, base=SAVED[number]):
            total[base + 8 * r : base + 8 * r + 8, :] = value

        level = 4 - number
        transfer_rows(region_k, same.at[level], cross.at[level], side, 8, store)
    before = jnp.maximum(narrow_at - 1, 0) * CHUNK_NARROW
    after = jnp.minimum(narrow_at + 1, 7) * CHUNK_NARROW
    for number, (side, at) in enumerate(LEVELS):
        for start, there, first in ((before, narrow_at > 0, 0), (after, narrow_at < 7, side - 2)):
            for k in range(2):
                given = jnp.where(there, got[pl.ds(start + at + k * side, side), :], 0.0)
                rows = pl.ds(SAVED[number] + first + k, side, stride=8)
                total[rows, :] = total[rows, :] + given
    for number, ((side, _), out) in enumerate(zip(LEVELS, (out3, out2, out1))):
        for r in range(side):
            at = SAVED[number] + 8 * r
            out[r] = total[at : at + side, :]

    region[...] = jnp.zeros_like(region)
    for r in range(8):
        at = (r + 2) * PITCH + 4
        region[at : at + 4, :] = coarse[4 * r : 4 * r + 4, :]

    def store_coarse(r, value):
        outc[r] = value

    transfer_rows(region, same.at[0], cross.at[0], 8, 4, store_coarse)

    dc = lax.broadcasted_iota(jnp.int32, (8, LANES), 0) - 3
    col_ok = (dc >= -2 - narrow_at % 2) & (dc <= 3 - narrow_at % 2)
    far = (dc >= 2) | (dc <= -2)
    first = jnp.zeros((8, LANES), F32)
    second = jnp.zeros((8, LANES), F32)
    for dr in range(-3, 4):
        row_ok = (dr >= -2 - wide_at % 2) & (dr <= 3 - wide_at % 2)
        allowed = col_ok & row_ok
        if abs(dr) < 2:
            allowed = allowed & far
        s = grid[pl.ds((wide_at + dr + 3) * PITCH + narrow_at, 8), :]
        at = (dr + 3) * 7
        first = first + jnp.where(allowed, same[1, at : at + 8, :] * s, 0.0)
        second = second + jnp.where(allowed, cross[1, at : at + 8, :] * s, 0.0)
    own = first + pltpu.roll(second, 64, 1)
    out0[0] = jnp.sum(own, axis=0, keepdims=True)


def downward(*operands):
    shape = lambda *dims: jax.ShapeDtypeStruct(dims, F32)
    tall = lambda rows: pltpu.VMEM((rows, 128), F32)
    return pl.pallas_call(
        down_kernel,
        out_shape=(
            shape(1, 1, 128), shape(2, 2, 128), shape(4, 4, 128), shape(8, 8, 128),
            shape(8, 4, 128), shape(4, 2, 128),
        ),
        in_specs=[VMEM] * 9,
        out_specs=(VMEM,) * 6,
        scratch_shapes=[
            tall(12 * PITCH), tall(8 * PITCH), tall(6 * PITCH), tall(112), tall(22 * PITCH), tall(12 * PITCH),
            pltpu.VMEM((32, 512), F32), pltpu.VMEM((8, 512), F32), tall(32),
        ],
        name="downward",
    )(*operands)


def exchange(boxes, axis):
    return lax.all_to_all(boxes[:, None, :], axis, 0, 0, tiled=True)[:, 0, :]


def local(offsets, strengths, leaf_map, shift_matrices, transfer_diagonal):
    leaf, l3, l2, l1, send, w_two, same, cross = upward(
        offsets.reshape(2, GROUPS, LANES),
        strengths.reshape(2, GROUPS, LANES),
        leaf_map.reshape(GROUPS, LANES),
        transfer_diagonal,
        shift_matrices,
    )
    l3, l2, l1, got, w_two, same, cross = kept_near(
        l3, l2, l1, exchange(send, "wide"), w_two, same, cross
    )
    send, top, bottom = pack(l3, l2, l1, got, same, cross)
    top, bottom, got = kept_near(top, bottom, exchange(send, "narrow"))
    local_zero, local_one, local_two, local_three, coarse_local, top_grid = downward(
        l3, l2, l1, top, bottom, got, w_two, same, cross
    )
    return (
        leaf.reshape(32, 32, 128), local_zero, local_one, local_two, local_three,
        coarse_local, top_grid,
    )


def solution(mesh):
    return jax.shard_map(
        local,
        mesh=mesh,
        in_specs=(
            P(None, "wide", "narrow", None),
            P(None, "wide", "narrow", None),
            P("wide", "narrow", None),
            P(),
            P(),
        ),
        out_specs=(
            P("wide", "narrow", None),
            P("wide", "narrow", None),
            P("wide", "narrow", None),
            P("wide", "narrow", None),
            P("wide", "narrow", None),
            P(),
            P(),
        ),
        check_vma=False,
    )
```

```python
import jax
import jax.numpy as jnp
from jax import lax
from jax.experimental import pallas as pl
from jax.experimental.pallas import tpu as pltpu
from jax.sharding import PartitionSpec as P


LANES = 128
GROUPS = 64
CHUNKS = (16, 16, 16, 16)
LEAVES = 1024
ALL = ("wide", "narrow")
F32 = jnp.float32
BF16 = jnp.bfloat16
VMEM = pl.BlockSpec(memory_space=pltpu.VMEM)
ANY = pl.BlockSpec(memory_space=pl.ANY)
HALO_ROWS = 28


def near_memory(*dims, kind=F32):
    return pltpu.VMEM(dims, kind)


def kept_near(*arrays):
    return tuple(pltpu.with_memory_space_constraint(a, pltpu.VMEM) for a in arrays)


PARTS = 4


def write_leaves(leaf, leaf_out, sem):
    rows = LEAVES // PARTS
    copies = [
        pltpu.make_async_copy(leaf.at[pl.ds(i * rows, rows)], leaf_out.at[pl.ds(i * rows, rows)], sem.at[i])
        for i in range(PARTS)
    ]
    for copy in copies:
        copy.start()
    return copies


def split_weights(src, dst):
    for quarter in range(4):
        rows = slice(quarter * 128, (quarter + 1) * 128)
        w = src[quarter]
        high = w.astype(BF16)
        dst[rows, 0:128] = high
        dst[rows, 128:256] = (w - high.astype(F32)).astype(BF16)


def merge(x, weights):
    count = x.shape[0]
    high = x.astype(BF16).astype(F32)
    both = jnp.concatenate([high, x - high], axis=0).astype(BF16)
    y = jnp.dot(both, weights, preferred_element_type=F32)
    return y[:count, :128] + y[:count, 128:] + y[count:, :128] + y[count:, 128:]


def gather_children(src, dst, rows, cols):
    for row_bit in range(2):
        for col_bit in range(2):
            quarter = 2 * row_bit + col_bit
            lanes = slice(quarter * 128, (quarter + 1) * 128)
            for r in range(rows):
                start = (2 * r + row_bit) * 2 * cols + col_bit
                if cols > 1:
                    piece = src[pl.ds(start, cols, stride=2), :]
                else:
                    piece = src[start : start + 1, :]
                dst[r * cols : (r + 1) * cols, lanes] = piece


def make_factors(diag, same, cross):
    lane = lax.broadcasted_iota(jnp.int32, (8, LANES), 1)
    for at in (0, 8, 16, 24, 32, 40, 41):
        rows = diag[at : at + 8, :]
        turned = pltpu.roll(rows, 64, 1)
        same[at : at + 8, :] = jnp.where(lane < 64, rows, turned)
        cross[at : at + 8, :] = jnp.where(lane < 64, turned, -rows)


def up_kernel(
    off, strg, lmap, diag, shifts,
    leaf_out, l3_out, l2_out, l1_out, even_out, odd_out, l0_out, w_low, same, cross,
    cheb, back, even, odd, acc, leaf, w_raw, w_two, x4, l4, x3, x2, x1, x0, w_sem, o_sem,
):
    w_copy = pltpu.make_async_copy(shifts, w_raw, w_sem)
    w_copy.start()

    for i in range(2):
        a = off[i]
        t = [None] * 9
        t[0] = jnp.ones_like(a)
        t[1] = a
        t[2] = 2.0 * a * a - 1.0
        t[3] = 2.0 * t[2] * a - a
        t[4] = 2.0 * t[2] * t[2] - 1.0
        t[5] = 2.0 * t[3] * t[2] - a
        t[6] = 2.0 * t[3] * t[3] - 1.0
        t[7] = 2.0 * t[4] * t[3] - a
        t[8] = 2.0 * t[4] * t[4] - 1.0
        for j in range(9):
            cheb[i, j * GROUPS : (j + 1) * GROUPS, :] = t[j]
        for j in range(8):
            back[i, j * GROUPS : (j + 1) * GROUPS, :] = t[8 - j]

    def make_terms(g, out, j):
        blocks = []
        for i in range(2):
            now = cheb[i, pl.ds(g, 8, stride=GROUPS), :]
            before = back[i, pl.ds(g, 8, stride=GROUPS), :]
            twice = 2.0 * jnp.broadcast_to(cheb[i, pl.ds(8 * GROUPS + g, 1), :], (8, LANES))
            seq = [now]
            for _ in range(7):
                now, before = twice * now - before, now
                seq.append(now)
            blocks.append(seq)
        qr = jnp.broadcast_to(strg[0, pl.ds(g, 1), :], (8, LANES))
        qi = jnp.broadcast_to(strg[1, pl.ds(g, 1), :], (8, LANES))
        real = jnp.concatenate([qr * ca - qi * cb for ca, cb in zip(*blocks)], axis=0)
        imag = jnp.concatenate([qr * cb + qi * ca for ca, cb in zip(*blocks)], axis=0)
        whole = jnp.concatenate([real, imag], axis=0)
        high = whole.astype(BF16)
        lanes = slice(j * LANES, (j + 1) * LANES)
        out[0:128, lanes] = high
        out[128:256, lanes] = (whole - high.astype(F32)).astype(BF16)

    ids = lax.broadcasted_iota(jnp.int32, (256, LANES), 0).astype(F32).astype(BF16)
    one = jnp.ones((256, LANES), BF16)
    zero = jnp.zeros((256, LANES), BF16)

    def terms_of(groups, out):
        for j, g in enumerate(groups):
            make_terms(g, out, j)

    def sums_of(groups, right):
        lefts = []
        for g in groups:
            row = lmap[pl.ds(g, 1), :]
            parts = []
            for b in range(4):
                near = (row - 256 * b).astype(F32)
                near = jnp.broadcast_to(near, (256, LANES)).astype(BF16)
                parts.append(jnp.where(near == ids, one, zero))
            lefts.append(jnp.concatenate(parts, axis=0))
        left = jnp.concatenate(lefts, axis=1)
        return lax.dot_general(
            left, right[:, 0 : len(groups) * LANES], (((1,), (1,)), ((), ())),
            preferred_element_type=F32,
        )

    chunks, at = [], 0
    for size in CHUNKS:
        chunks.append(range(at, at + size))
        at += size
    buffers = (even, odd)
    terms_of(chunks[0], even)
    for level in range(5):
        make_factors(diag.at[level], same.at[level], cross.at[level])
    for k, groups in enumerate(chunks):
        if k + 1 < len(chunks):
            terms_of(chunks[k + 1], buffers[(k + 1) % 2])
        part = sums_of(groups, buffers[k % 2])
        if k == 0:
            acc[...] = part
        elif k + 1 < len(chunks):
            acc[...] += part
        else:
            part = acc[...] + part
            leaf[...] = part[:, 0:128] + part[:, 128:256]
    copies = write_leaves(leaf, leaf_out, o_sem)
    w_copy.wait()
    for t in range(7):
        split_weights(w_raw.at[t], w_low.at[t] if t < 2 else w_two.at[t - 2])

    gather_children(leaf, x4, 16, 16)
    l4[...] = merge(x4[...], w_two[4])
    gather_children(l4, x3, 8, 8)
    l3_out[...] = merge(x3[...], w_two[3])
    gather_children(l3_out, x2, 4, 4)
    l2_out[...] = merge(x2[...], w_two[2])
    gather_children(l2_out, x1, 2, 2)
    l1_out[...] = merge(x1[...], w_two[1])
    gather_children(l1_out, x0, 1, 1)
    root = merge(x0[...], w_two[0])[0:1]
    l0_out[...] = jnp.broadcast_to(root, (128, LANES))
    is_odd = lax.axis_index("wide") % 2 == 1
    for at, rows, up_value, down_value in (
        (0, 16, l3_out[0:16, :], l3_out[48:64, :]), (16, 8, l2_out[0:8, :], l2_out[8:16, :]),
    ):
        even_out[at : at + rows, :] = jnp.where(is_odd, up_value, down_value)
        odd_out[at : at + rows, :] = jnp.where(is_odd, down_value, up_value)
    even_out[24:28, :] = l1_out[0:4, :]
    odd_out[24:28, :] = l1_out[0:4, :]

    for copy in copies:
        copy.wait()


def upward(*operands):
    scratch = lambda dims, kind=F32: pltpu.VMEM(dims, kind)
    return pl.pallas_call(
        up_kernel,
        out_shape=(
            jax.ShapeDtypeStruct((LEAVES, 128), F32), near_memory(64, 128), near_memory(16, 128),
            near_memory(8, 128), near_memory(HALO_ROWS, 128), near_memory(HALO_ROWS, 128),
            near_memory(128, 128),
            near_memory(2, 512, 256, kind=BF16), near_memory(5, 56, 128), near_memory(5, 56, 128),
        ),
        in_specs=[VMEM, VMEM, VMEM, VMEM, ANY],
        out_specs=(ANY,) + (VMEM,) * 9,
        scratch_shapes=[
            scratch((2, 9 * GROUPS, LANES)),
            scratch((2, 8 * GROUPS, LANES)),
            scratch((256, max(CHUNKS) * LANES), BF16),
            scratch((256, max(CHUNKS) * LANES), BF16),
            scratch((LEAVES, 256)),
            scratch((LEAVES, 128)),
            scratch((7, 4, 128, 128)),
            scratch((5, 512, 256), BF16),
            scratch((256, 512)),
            scratch((256, 128)),
            scratch((64, 512)),
            scratch((16, 512)),
            scratch((8, 512)),
            scratch((8, 512)),
            pltpu.SemaphoreType.DMA,
            pltpu.SemaphoreType.DMA((PARTS,)),
        ],
        name="upward",
    )(*operands)


PITCH = 16
LEVELS = ((8, 0), (4, 16), (2, 24))
SAVED = (0, 64, 96)


def transfer_rows(region, same, cross, side, cols, store):
    odd = (lax.broadcasted_iota(jnp.int32, (8, LANES), 0) % 2) == 1

    def factor(table, dr, dc):
        at = (dr + 3) * 7 + 3
        if dc < 3:
            return jnp.broadcast_to(table[at + dc : at + dc + 1, :], (8, LANES))
        right = jnp.broadcast_to(table[at + 3 : at + 4, :], (8, LANES))
        left = jnp.broadcast_to(table[at - 3 : at - 2, :], (8, LANES))
        return jnp.where(odd, left, right)

    def source(row, dc):
        base = row * PITCH + 4
        if dc < 3:
            return region[base + dc : base + dc + 8, :]
        return jnp.where(odd, region[base - 3 : base + 5, :], region[base + 3 : base + 11, :])

    for r in range(side):
        first = jnp.zeros((8, LANES), F32)
        second = jnp.zeros((8, LANES), F32)
        for dr in range(-2 - r % 2, 4 - r % 2):
            for dc in (-2, -1, 0, 1, 2, 3):
                if max(abs(dr), abs(dc)) < 2:
                    continue
                s = source(r + dr + 2, dc)
                first = first + factor(same, dr, dc) * s
                second = second + factor(cross, dr, dc) * s
        store(r, (first + pltpu.roll(second, 64, 1))[0:cols])


def column_products(column, same, cross, dcs):
    odd = (lax.broadcasted_iota(jnp.int32, (8, LANES), 0) % 2) == 1
    first = jnp.zeros((8, LANES), F32)
    second = jnp.zeros((8, LANES), F32)

    def factor(table, dr, dc):
        at = (dr + 3) * 7 + dc + 3
        if dr < 3:
            return jnp.broadcast_to(table[at : at + 1, :], (8, LANES))
        low = jnp.broadcast_to(table[dc + 3 : dc + 4, :], (8, LANES))
        high = jnp.broadcast_to(table[at : at + 1, :], (8, LANES))
        return jnp.where(odd, low, high)

    for k, dc in enumerate(dcs):
        for dr in (-2, -1, 0, 1, 2, 3):
            if max(abs(dr), abs(dc)) < 2:
                continue
            at = k * PITCH + 4
            if dr < 3:
                s = column[at + dr : at + dr + 8, :]
            else:
                s = jnp.where(odd, column[at - 3 : at + 5, :], column[at + 3 : at + 11, :])
            first = first + factor(same, dr, dc) * s
            second = second + factor(cross, dr, dc) * s
    return first + pltpu.roll(second, 64, 1)


def pack_kernel(
    l3, l2, l1, even, odd, same, cross, even_out, odd_out, top, bottom, columns, west_out, east_out
):
    is_odd = lax.axis_index("wide") % 2 == 1
    top[...] = jnp.where(is_odd, even[...], odd[...])
    bottom[...] = jnp.where(is_odd, odd[...], even[...])
    for number, (grid, (side, row_at)) in enumerate(zip((l3, l2, l1), LEVELS)):
        level = 4 - number
        for east in range(2):
            column = columns.at[2 * number + east]
            for k in range(2):
                c = k + east * (side - 2)
                at = k * PITCH + 2
                column[at : at + 2, :] = top[pl.ds(row_at + c, 2, stride=side), :]
                column[at + 2 : at + 2 + side, :] = grid[pl.ds(c, side, stride=side), :]
                column[at + 2 + side : at + 4 + side, :] = bottom[pl.ds(row_at + c, 2, stride=side), :]
            for target, dcs in enumerate(((-2, -1), (-3, -2)) if east else ((2, 3), (1, 2))):
                value = column_products(column, same.at[level], cross.at[level], dcs)
                out = east_out if east else west_out
                at = row_at + target * side
                out[at : at + side, :] = value[0:side]
    is_odd = lax.axis_index("narrow") % 2 == 1
    even_out[...] = jnp.where(is_odd, west_out[...], east_out[...])
    odd_out[...] = jnp.where(is_odd, east_out[...], west_out[...])


def pack(*operands):
    return pl.pallas_call(
        pack_kernel,
        out_shape=(near_memory(HALO_ROWS, 128),) * 4,
        in_specs=[VMEM] * 7,
        out_specs=(VMEM,) * 4,
        scratch_shapes=[
            pltpu.VMEM((6, 2 * PITCH, 128), F32), pltpu.VMEM((HALO_ROWS, 128), F32),
            pltpu.VMEM((HALO_ROWS, 128), F32),
        ],
        name="pack",
    )(*operands)


def near_kernel(l3, l2, l1, top, bottom, same, cross, saved, other, r3, r2, r1):
    other[...] = jnp.zeros_like(other)
    for number, (own, region_k, (side, row_at)) in enumerate(
        zip((l3, l2, l1), (r3, r2, r1), LEVELS)
    ):
        region_k[...] = jnp.zeros_like(region_k)
        for r in range(side):
            at = (r + 2) * PITCH + 4
            region_k[at : at + side, :] = own[r * side : (r + 1) * side, :]
        for r in range(2):
            at = r * PITCH + 4
            region_k[at : at + side, :] = top[row_at + r * side : row_at + (r + 1) * side, :]
            at = (r + 2 + side) * PITCH + 4
            region_k[at : at + side, :] = bottom[row_at + r * side : row_at + (r + 1) * side, :]

        def store(r, value, base=SAVED[number]):
            saved[base + 8 * r : base + 8 * r + 8, :] = value

        level = 4 - number
        transfer_rows(region_k, same.at[level], cross.at[level], side, 8, store)


def near(*operands):
    tall = lambda rows: pltpu.VMEM((rows, 128), F32)
    return pl.pallas_call(
        near_kernel,
        out_shape=(near_memory(112, 128), near_memory(8, 128)),
        in_specs=[VMEM] * 7,
        out_specs=(VMEM,) * 2,
        scratch_shapes=[tall(12 * PITCH), tall(8 * PITCH), tall(6 * PITCH)],
        name="near",
    )(*operands)


def down_kernel(
    saved, even, odd, roots, w_two, same, cross,
    out0, out1, out2, out3, outc, outt,
    total, grid, region, xc, xt, coarse, west, east,
):
    wide_at = lax.axis_index("wide")
    narrow_at = lax.axis_index("narrow")
    grid[...] = jnp.zeros_like(grid)
    for r in range(16):
        at = (r + 3) * PITCH + 3
        grid[at : at + 8, :] = roots[r * 8 : (r + 1) * 8, :]
    for row_bit in range(2):
        for col_bit in range(2):
            lanes = slice((2 * row_bit + col_bit) * 128, (2 * row_bit + col_bit + 1) * 128)
            for r in range(8):
                at = (2 * r + row_bit + 3) * PITCH + 3 + col_bit
                xc[4 * r : 4 * r + 4, lanes] = grid[pl.ds(at, 4, stride=2), :]
    coarse[...] = merge(xc[...], w_two[1])
    gather_children(coarse, xt, 4, 2)
    peak = merge(xt[...], w_two[0])
    for r in range(4):
        outt[r] = peak[2 * r : 2 * r + 2]

    is_odd = narrow_at % 2 == 1
    west[...] = jnp.where(is_odd, even[...], odd[...])
    east[...] = jnp.where(is_odd, odd[...], even[...])
    total[...] = saved[...]
    for number, (side, at) in enumerate(LEVELS):
        for given, first in ((west, 0), (east, side - 2)):
            for k in range(2):
                rows = pl.ds(SAVED[number] + first + k, side, stride=8)
                total[rows, :] = total[rows, :] + given[at + k * side : at + (k + 1) * side, :]
    for number, ((side, _), out) in enumerate(zip(LEVELS, (out3, out2, out1))):
        for r in range(side):
            at = SAVED[number] + 8 * r
            out[r] = total[at : at + side, :]

    region[...] = jnp.zeros_like(region)
    for r in range(8):
        at = (r + 2) * PITCH + 4
        region[at : at + 4, :] = coarse[4 * r : 4 * r + 4, :]

    def store_coarse(r, value):
        outc[r] = value

    transfer_rows(region, same.at[0], cross.at[0], 8, 4, store_coarse)

    dc = lax.broadcasted_iota(jnp.int32, (8, LANES), 0) - 3
    col_ok = (dc >= -2 - narrow_at % 2) & (dc <= 3 - narrow_at % 2)
    far = (dc >= 2) | (dc <= -2)
    first = jnp.zeros((8, LANES), F32)
    second = jnp.zeros((8, LANES), F32)
    for dr in range(-3, 4):
        row_ok = (dr >= -2 - wide_at % 2) & (dr <= 3 - wide_at % 2)
        allowed = col_ok & row_ok
        if abs(dr) < 2:
            allowed = allowed & far
        s = grid[pl.ds((wide_at + dr + 3) * PITCH + narrow_at, 8), :]
        at = (dr + 3) * 7
        first = first + jnp.where(allowed, same[1, at : at + 8, :] * s, 0.0)
        second = second + jnp.where(allowed, cross[1, at : at + 8, :] * s, 0.0)
    own = first + pltpu.roll(second, 64, 1)
    out0[0] = jnp.sum(own, axis=0, keepdims=True)


def downward(*operands):
    shape = lambda *dims: jax.ShapeDtypeStruct(dims, F32)
    tall = lambda rows: pltpu.VMEM((rows, 128), F32)
    return pl.pallas_call(
        down_kernel,
        out_shape=(
            shape(1, 1, 128), shape(2, 2, 128), shape(4, 4, 128), shape(8, 8, 128),
            shape(8, 4, 128), shape(4, 2, 128),
        ),
        in_specs=[VMEM] * 7,
        out_specs=(VMEM,) * 6,
        scratch_shapes=[
            tall(112), tall(22 * PITCH), tall(12 * PITCH),
            pltpu.VMEM((32, 512), F32), pltpu.VMEM((8, 512), F32), tall(32),
            tall(HALO_ROWS), tall(HALO_ROWS),
        ],
        name="downward",
    )(*operands)


def exchange(boxes, axis):
    return lax.all_to_all(boxes[:, None, :], axis, 0, 0, tiled=True)[:, 0, :]


def swap_pairs(x, axis, first):
    lower = range(first, lax.axis_size(axis) - 1, 2)
    pairs = [pair for i in lower for pair in ((i, i + 1), (i + 1, i))]
    return lax.ppermute(x, axis, pairs)


def steps(offsets, strengths, leaf_map, shift_matrices, transfer_diagonal):
    leaf, l3, l2, l1, even, odd, root, w_two, same, cross = upward(
        offsets.reshape(2, GROUPS, LANES),
        strengths.reshape(2, GROUPS, LANES),
        leaf_map.reshape(GROUPS, LANES),
        transfer_diagonal,
        shift_matrices,
    )
    odd = swap_pairs(odd, "wide", 1)
    even = swap_pairs(even, "wide", 0)
    roots = exchange(root, ALL)
    l3, l2, l1, w_two, same, cross, even, odd = kept_near(
        l3, l2, l1, w_two, same, cross, even, odd
    )
    even, odd, top, bottom = pack(l3, l2, l1, even, odd, same, cross)
    odd = swap_pairs(odd, "narrow", 1)
    even = swap_pairs(even, "narrow", 0)
    top, bottom = kept_near(top, bottom)
    saved, _ = near(l3, l2, l1, top, bottom, same, cross)
    local_zero, local_one, local_two, local_three, coarse_local, top_grid = downward(
        *kept_near(saved, even, odd, roots), w_two, same, cross
    )
    return (
        leaf.reshape(32, 32, 128), local_zero, local_one, local_two, local_three,
        coarse_local, top_grid,
    )


def solution(mesh):
    return jax.shard_map(
        steps,
        mesh=mesh,
        in_specs=(
            P(None, "wide", "narrow", None),
            P(None, "wide", "narrow", None),
            P("wide", "narrow", None),
            P(),
            P(),
        ),
        out_specs=(
            P("wide", "narrow", None),
            P("wide", "narrow", None),
            P("wide", "narrow", None),
            P("wide", "narrow", None),
            P("wide", "narrow", None),
            P(),
            P(),
        ),
        check_vma=False,
    )
```

```python
import jax
import jax.numpy as jnp
from jax import lax
from jax.experimental import pallas as pl
from jax.experimental.pallas import tpu as pltpu
from jax.sharding import PartitionSpec as P


LANES = 128
GROUPS = 64
CHUNKS = (2, 62)
LEAVES = 1024
ALL = ("wide", "narrow")
F32 = jnp.float32
BF16 = jnp.bfloat16
VMEM = pl.BlockSpec(memory_space=pltpu.VMEM)
ANY = pl.BlockSpec(memory_space=pl.ANY)
HALO_ROWS = 28


def near_memory(*dims, kind=F32):
    return pltpu.VMEM(dims, kind)


def kept_near(*arrays):
    return tuple(pltpu.with_memory_space_constraint(a, pltpu.VMEM) for a in arrays)


PARTS = 4


def write_leaves(leaf, leaf_out, sem):
    rows = LEAVES // PARTS
    copies = [
        pltpu.make_async_copy(leaf.at[pl.ds(i * rows, rows)], leaf_out.at[pl.ds(i * rows, rows)], sem.at[i])
        for i in range(PARTS)
    ]
    for copy in copies:
        copy.start()
    return copies


def split_weights(src, dst):
    for quarter in range(4):
        rows = slice(quarter * 128, (quarter + 1) * 128)
        w = src[quarter]
        high = w.astype(BF16)
        dst[rows, 0:128] = high
        dst[rows, 128:256] = (w - high.astype(F32)).astype(BF16)


def merge(x, weights):
    count = x.shape[0]
    high = x.astype(BF16).astype(F32)
    both = jnp.concatenate([high, x - high], axis=0).astype(BF16)
    y = jnp.dot(both, weights, preferred_element_type=F32)
    return y[:count, :128] + y[:count, 128:] + y[count:, :128] + y[count:, 128:]


def gather_children(src, dst, rows, cols):
    for row_bit in range(2):
        for col_bit in range(2):
            quarter = 2 * row_bit + col_bit
            lanes = slice(quarter * 128, (quarter + 1) * 128)
            for r in range(rows):
                start = (2 * r + row_bit) * 2 * cols + col_bit
                if cols > 1:
                    piece = src[pl.ds(start, cols, stride=2), :]
                else:
                    piece = src[start : start + 1, :]
                dst[r * cols : (r + 1) * cols, lanes] = piece


def make_factors(diag, same, cross):
    lane = lax.broadcasted_iota(jnp.int32, (8, LANES), 1)
    for at in (0, 8, 16, 24, 32, 40, 41):
        rows = diag[at : at + 8, :]
        turned = pltpu.roll(rows, 64, 1)
        same[at : at + 8, :] = jnp.where(lane < 64, rows, turned)
        cross[at : at + 8, :] = jnp.where(lane < 64, turned, -rows)


def up_kernel(
    off, strg, lmap, diag, shifts,
    leaf_out, l3_out, l2_out, l1_out, even_out, odd_out, root_out, w_low, same, cross,
    cheb, back, even, odd, acc, leaf, w_raw, w_two, x4, l4, x3, x2, x1, x0, l0, w_sem, o_sem, r_sem,
):
    w_copy = pltpu.make_async_copy(shifts, w_raw, w_sem)
    w_copy.start()

    for i in range(2):
        a = off[i]
        t = [None] * 9
        t[0] = jnp.ones_like(a)
        t[1] = a
        t[2] = 2.0 * a * a - 1.0
        t[3] = 2.0 * t[2] * a - a
        t[4] = 2.0 * t[2] * t[2] - 1.0
        t[5] = 2.0 * t[3] * t[2] - a
        t[6] = 2.0 * t[3] * t[3] - 1.0
        t[7] = 2.0 * t[4] * t[3] - a
        t[8] = 2.0 * t[4] * t[4] - 1.0
        for j in range(9):
            cheb[i, j * GROUPS : (j + 1) * GROUPS, :] = t[j]
        for j in range(8):
            back[i, j * GROUPS : (j + 1) * GROUPS, :] = t[8 - j]

    def make_terms(g, out, j):
        blocks = []
        for i in range(2):
            now = cheb[i, pl.ds(g, 8, stride=GROUPS), :]
            before = back[i, pl.ds(g, 8, stride=GROUPS), :]
            twice = 2.0 * jnp.broadcast_to(cheb[i, pl.ds(8 * GROUPS + g, 1), :], (8, LANES))
            seq = [now]
            for _ in range(7):
                now, before = twice * now - before, now
                seq.append(now)
            blocks.append(seq)
        qr = jnp.broadcast_to(strg[0, pl.ds(g, 1), :], (8, LANES))
        qi = jnp.broadcast_to(strg[1, pl.ds(g, 1), :], (8, LANES))
        real = jnp.concatenate([qr * ca - qi * cb for ca, cb in zip(*blocks)], axis=0)
        imag = jnp.concatenate([qr * cb + qi * ca for ca, cb in zip(*blocks)], axis=0)
        whole = jnp.concatenate([real, imag], axis=0)
        high = whole.astype(BF16)
        lanes = slice(j * LANES, (j + 1) * LANES)
        out[0:128, lanes] = high
        out[128:256, lanes] = (whole - high.astype(F32)).astype(BF16)

    ids = lax.broadcasted_iota(jnp.int32, (256, LANES), 0).astype(F32).astype(BF16)
    one = jnp.ones((256, LANES), BF16)
    zero = jnp.zeros((256, LANES), BF16)

    def terms_of(groups, out):
        for j, g in enumerate(groups):
            make_terms(g, out, j)

    def sums_of(groups, right):
        lefts = []
        for g in groups:
            row = lmap[pl.ds(g, 1), :]
            parts = []
            for b in range(4):
                near = (row - 256 * b).astype(F32)
                near = jnp.broadcast_to(near, (256, LANES)).astype(BF16)
                parts.append(jnp.where(near == ids, one, zero))
            lefts.append(jnp.concatenate(parts, axis=0))
        left = jnp.concatenate(lefts, axis=1)
        return lax.dot_general(
            left, right[:, 0 : len(groups) * LANES], (((1,), (1,)), ((), ())),
            preferred_element_type=F32,
        )

    chunks, at = [], 0
    for size in CHUNKS:
        chunks.append(range(at, at + size))
        at += size
    buffers = (even, odd)
    terms_of(chunks[0], even)
    for level in range(5):
        make_factors(diag.at[level], same.at[level], cross.at[level])
    for k, groups in enumerate(chunks):
        if k + 1 < len(chunks):
            terms_of(chunks[k + 1], buffers[(k + 1) % 2])
        part = sums_of(groups, buffers[k % 2])
        if k == 0:
            acc[...] = part
        elif k + 1 < len(chunks):
            acc[...] += part
        else:
            part = acc[...] + part
            leaf[...] = part[:, 0:128] + part[:, 128:256]
    copies = write_leaves(leaf, leaf_out, o_sem)
    w_copy.wait()
    for t in range(7):
        split_weights(w_raw.at[t], w_low.at[t] if t < 2 else w_two.at[t - 2])

    gather_children(leaf, x4, 16, 16)
    l4[...] = merge(x4[...], w_two[4])
    gather_children(l4, x3, 8, 8)
    l3_out[...] = merge(x3[...], w_two[3])
    gather_children(l3_out, x2, 4, 4)
    l2_out[...] = merge(x2[...], w_two[2])
    gather_children(l2_out, x1, 2, 2)
    l1_out[...] = merge(x1[...], w_two[1])
    gather_children(l1_out, x0, 1, 1)
    root = merge(x0[...], w_two[0])[0:1]
    l0[...] = jnp.broadcast_to(root, (128, LANES))
    copies.append(pltpu.make_async_copy(l0, root_out, r_sem))
    copies[-1].start()
    is_odd = lax.axis_index("wide") % 2 == 1
    for at, rows, up_value, down_value in (
        (0, 16, l3_out[0:16, :], l3_out[48:64, :]), (16, 8, l2_out[0:8, :], l2_out[8:16, :]),
    ):
        even_out[at : at + rows, :] = jnp.where(is_odd, up_value, down_value)
        odd_out[at : at + rows, :] = jnp.where(is_odd, down_value, up_value)
    even_out[24:28, :] = l1_out[0:4, :]
    odd_out[24:28, :] = l1_out[0:4, :]

    for copy in copies:
        copy.wait()


def upward(*operands):
    scratch = lambda dims, kind=F32: pltpu.VMEM(dims, kind)
    return pl.pallas_call(
        up_kernel,
        out_shape=(
            jax.ShapeDtypeStruct((LEAVES, 128), F32), near_memory(64, 128), near_memory(16, 128),
            near_memory(8, 128), near_memory(HALO_ROWS, 128), near_memory(HALO_ROWS, 128),
            jax.ShapeDtypeStruct((128, 128), F32),
            near_memory(2, 512, 256, kind=BF16), near_memory(5, 56, 128), near_memory(5, 56, 128),
        ),
        in_specs=[VMEM, VMEM, VMEM, VMEM, ANY],
        out_specs=(ANY,) + (VMEM,) * 5 + (ANY,) + (VMEM,) * 3,
        scratch_shapes=[
            scratch((2, 9 * GROUPS, LANES)),
            scratch((2, 8 * GROUPS, LANES)),
            scratch((256, max(CHUNKS) * LANES), BF16),
            scratch((256, max(CHUNKS) * LANES), BF16),
            scratch((LEAVES, 256)),
            scratch((LEAVES, 128)),
            scratch((7, 4, 128, 128)),
            scratch((5, 512, 256), BF16),
            scratch((256, 512)),
            scratch((256, 128)),
            scratch((64, 512)),
            scratch((16, 512)),
            scratch((8, 512)),
            scratch((8, 512)),
            scratch((128, 128)),
            pltpu.SemaphoreType.DMA,
            pltpu.SemaphoreType.DMA((PARTS,)),
            pltpu.SemaphoreType.DMA,
        ],
        name="upward",
    )(*operands)


PITCH = 16
LEVELS = ((8, 0), (4, 16), (2, 24))
SAVED = (0, 64, 96)


def transfer_rows(region, same, cross, side, cols, store):
    odd = (lax.broadcasted_iota(jnp.int32, (8, LANES), 0) % 2) == 1

    def factor(table, dr, dc):
        at = (dr + 3) * 7 + 3
        if dc < 3:
            return jnp.broadcast_to(table[at + dc : at + dc + 1, :], (8, LANES))
        right = jnp.broadcast_to(table[at + 3 : at + 4, :], (8, LANES))
        left = jnp.broadcast_to(table[at - 3 : at - 2, :], (8, LANES))
        return jnp.where(odd, left, right)

    def source(row, dc):
        base = row * PITCH + 4
        if dc < 3:
            return region[base + dc : base + dc + 8, :]
        return jnp.where(odd, region[base - 3 : base + 5, :], region[base + 3 : base + 11, :])

    for r in range(side):
        first = jnp.zeros((8, LANES), F32)
        second = jnp.zeros((8, LANES), F32)
        for dr in range(-2 - r % 2, 4 - r % 2):
            for dc in (-2, -1, 0, 1, 2, 3):
                if max(abs(dr), abs(dc)) < 2:
                    continue
                s = source(r + dr + 2, dc)
                first = first + factor(same, dr, dc) * s
                second = second + factor(cross, dr, dc) * s
        store(r, (first + pltpu.roll(second, 64, 1))[0:cols])


def column_products(column, same, cross, dcs):
    odd = (lax.broadcasted_iota(jnp.int32, (8, LANES), 0) % 2) == 1
    first = jnp.zeros((8, LANES), F32)
    second = jnp.zeros((8, LANES), F32)

    def factor(table, dr, dc):
        at = (dr + 3) * 7 + dc + 3
        if dr < 3:
            return jnp.broadcast_to(table[at : at + 1, :], (8, LANES))
        low = jnp.broadcast_to(table[dc + 3 : dc + 4, :], (8, LANES))
        high = jnp.broadcast_to(table[at : at + 1, :], (8, LANES))
        return jnp.where(odd, low, high)

    for k, dc in enumerate(dcs):
        for dr in (-2, -1, 0, 1, 2, 3):
            if max(abs(dr), abs(dc)) < 2:
                continue
            at = k * PITCH + 4
            if dr < 3:
                s = column[at + dr : at + dr + 8, :]
            else:
                s = jnp.where(odd, column[at - 3 : at + 5, :], column[at + 3 : at + 11, :])
            first = first + factor(same, dr, dc) * s
            second = second + factor(cross, dr, dc) * s
    return first + pltpu.roll(second, 64, 1)


def pack_kernel(
    l3, l2, l1, even, odd, same, cross, even_out, odd_out, top, bottom, columns, west_out, east_out
):
    is_odd = lax.axis_index("wide") % 2 == 1
    top[...] = jnp.where(is_odd, even[...], odd[...])
    bottom[...] = jnp.where(is_odd, odd[...], even[...])
    for number, (grid, (side, row_at)) in enumerate(zip((l3, l2, l1), LEVELS)):
        level = 4 - number
        for east in range(2):
            column = columns.at[2 * number + east]
            for k in range(2):
                c = k + east * (side - 2)
                at = k * PITCH + 2
                column[at : at + 2, :] = top[pl.ds(row_at + c, 2, stride=side), :]
                column[at + 2 : at + 2 + side, :] = grid[pl.ds(c, side, stride=side), :]
                column[at + 2 + side : at + 4 + side, :] = bottom[pl.ds(row_at + c, 2, stride=side), :]
            for target, dcs in enumerate(((-2, -1), (-3, -2)) if east else ((2, 3), (1, 2))):
                value = column_products(column, same.at[level], cross.at[level], dcs)
                out = east_out if east else west_out
                at = row_at + target * side
                out[at : at + side, :] = value[0:side]
    is_odd = lax.axis_index("narrow") % 2 == 1
    even_out[...] = jnp.where(is_odd, west_out[...], east_out[...])
    odd_out[...] = jnp.where(is_odd, east_out[...], west_out[...])


def pack(*operands):
    return pl.pallas_call(
        pack_kernel,
        out_shape=(near_memory(HALO_ROWS, 128),) * 4,
        in_specs=[VMEM] * 7,
        out_specs=(VMEM,) * 4,
        scratch_shapes=[
            pltpu.VMEM((6, 2 * PITCH, 128), F32), pltpu.VMEM((HALO_ROWS, 128), F32),
            pltpu.VMEM((HALO_ROWS, 128), F32),
        ],
        name="pack",
    )(*operands)


def near_kernel(l3, l2, l1, top, bottom, same, cross, saved3, saved21, r3, r2, r1):
    for number, (own, region_k, (side, row_at)) in enumerate(
        zip((l3, l2, l1), (r3, r2, r1), LEVELS)
    ):
        region_k[...] = jnp.zeros_like(region_k)
        for r in range(side):
            at = (r + 2) * PITCH + 4
            region_k[at : at + side, :] = own[r * side : (r + 1) * side, :]
        for r in range(2):
            at = r * PITCH + 4
            region_k[at : at + side, :] = top[row_at + r * side : row_at + (r + 1) * side, :]
            at = (r + 2 + side) * PITCH + 4
            region_k[at : at + side, :] = bottom[row_at + r * side : row_at + (r + 1) * side, :]

        def store(r, value, saved=saved21 if number else saved3, base=SAVED[number] - 64 * min(number, 1)):
            saved[base + 8 * r : base + 8 * r + 8, :] = value

        level = 4 - number
        transfer_rows(region_k, same.at[level], cross.at[level], side, 8, store)


def near(*operands):
    tall = lambda rows: pltpu.VMEM((rows, 128), F32)
    return pl.pallas_call(
        near_kernel,
        out_shape=(near_memory(64, 128), near_memory(48, 128)),
        in_specs=[VMEM] * 7,
        out_specs=(VMEM,) * 2,
        scratch_shapes=[tall(12 * PITCH), tall(8 * PITCH), tall(6 * PITCH)],
        name="near",
    )(*operands)


def down_kernel(
    saved3, saved21, even, odd, roots, w_two, same, cross,
    out0, out1, out2, out3, outc, outt,
    total, grid, region, xc, xt, coarse, west, east,
):
    wide_at = lax.axis_index("wide")
    narrow_at = lax.axis_index("narrow")
    grid[...] = jnp.zeros_like(grid)
    for r in range(16):
        at = (r + 3) * PITCH + 3
        grid[at : at + 8, :] = roots[r * 8 : (r + 1) * 8, :]
    for row_bit in range(2):
        for col_bit in range(2):
            lanes = slice((2 * row_bit + col_bit) * 128, (2 * row_bit + col_bit + 1) * 128)
            for r in range(8):
                at = (2 * r + row_bit + 3) * PITCH + 3 + col_bit
                xc[4 * r : 4 * r + 4, lanes] = grid[pl.ds(at, 4, stride=2), :]
    coarse[...] = merge(xc[...], w_two[1])
    gather_children(coarse, xt, 4, 2)
    peak = merge(xt[...], w_two[0])
    for r in range(4):
        outt[r] = peak[2 * r : 2 * r + 2]

    is_odd = narrow_at % 2 == 1
    west[...] = jnp.where(is_odd, even[...], odd[...])
    east[...] = jnp.where(is_odd, odd[...], even[...])
    total[0:64, :] = saved3[...]
    total[64:112, :] = saved21[...]
    for number, (side, at) in enumerate(LEVELS):
        for given, first in ((west, 0), (east, side - 2)):
            for k in range(2):
                rows = pl.ds(SAVED[number] + first + k, side, stride=8)
                total[rows, :] = total[rows, :] + given[at + k * side : at + (k + 1) * side, :]
    for number, ((side, _), out) in enumerate(zip(LEVELS, (out3, out2, out1))):
        for r in range(side):
            at = SAVED[number] + 8 * r
            out[r] = total[at : at + side, :]

    region[...] = jnp.zeros_like(region)
    for r in range(8):
        at = (r + 2) * PITCH + 4
        region[at : at + 4, :] = coarse[4 * r : 4 * r + 4, :]

    def store_coarse(r, value):
        outc[r] = value

    transfer_rows(region, same.at[0], cross.at[0], 8, 4, store_coarse)

    dc = lax.broadcasted_iota(jnp.int32, (8, LANES), 0) - 3
    col_ok = (dc >= -2 - narrow_at % 2) & (dc <= 3 - narrow_at % 2)
    far = (dc >= 2) | (dc <= -2)
    first = jnp.zeros((8, LANES), F32)
    second = jnp.zeros((8, LANES), F32)
    for dr in range(-3, 4):
        row_ok = (dr >= -2 - wide_at % 2) & (dr <= 3 - wide_at % 2)
        allowed = col_ok & row_ok
        if abs(dr) < 2:
            allowed = allowed & far
        s = grid[pl.ds((wide_at + dr + 3) * PITCH + narrow_at, 8), :]
        at = (dr + 3) * 7
        first = first + jnp.where(allowed, same[1, at : at + 8, :] * s, 0.0)
        second = second + jnp.where(allowed, cross[1, at : at + 8, :] * s, 0.0)
    own = first + pltpu.roll(second, 64, 1)
    out0[0] = jnp.sum(own, axis=0, keepdims=True)


def downward(*operands):
    shape = lambda *dims: jax.ShapeDtypeStruct(dims, F32)
    tall = lambda rows: pltpu.VMEM((rows, 128), F32)
    return pl.pallas_call(
        down_kernel,
        out_shape=(
            shape(1, 1, 128), shape(2, 2, 128), shape(4, 4, 128), shape(8, 8, 128),
            shape(8, 4, 128), shape(4, 2, 128),
        ),
        in_specs=[VMEM] * 8,
        out_specs=(VMEM,) * 6,
        scratch_shapes=[
            tall(112), tall(22 * PITCH), tall(12 * PITCH),
            pltpu.VMEM((32, 512), F32), pltpu.VMEM((8, 512), F32), tall(32),
            tall(HALO_ROWS), tall(HALO_ROWS),
        ],
        name="downward",
    )(*operands)


def exchange(boxes, axis):
    return lax.all_to_all(boxes[:, None, :], axis, 0, 0, tiled=True)[:, 0, :]


def swap_pairs(x, axis, first):
    lower = range(first, lax.axis_size(axis) - 1, 2)
    pairs = [pair for i in lower for pair in ((i, i + 1), (i + 1, i))]
    return lax.ppermute(x, axis, pairs)


def steps(offsets, strengths, leaf_map, shift_matrices, transfer_diagonal):
    leaf, l3, l2, l1, even, odd, root, w_two, same, cross = upward(
        offsets.reshape(2, GROUPS, LANES),
        strengths.reshape(2, GROUPS, LANES),
        leaf_map.reshape(GROUPS, LANES),
        transfer_diagonal,
        shift_matrices,
    )
    odd = swap_pairs(odd, "wide", 1)
    even = swap_pairs(even, "wide", 0)
    roots = exchange(root, ALL)
    l3, l2, l1, w_two, same, cross, even, odd = kept_near(
        l3, l2, l1, w_two, same, cross, even, odd
    )
    even, odd, top, bottom = pack(l3, l2, l1, even, odd, same, cross)
    odd = swap_pairs(odd, "narrow", 1)
    even = swap_pairs(even, "narrow", 0)
    top, bottom = kept_near(top, bottom)
    saved = near(l3, l2, l1, top, bottom, same, cross)
    local_zero, local_one, local_two, local_three, coarse_local, top_grid = downward(
        *kept_near(*saved, even, odd, roots), w_two, same, cross
    )
    return (
        leaf.reshape(32, 32, 128), local_zero, local_one, local_two, local_three,
        coarse_local, top_grid,
    )


def solution(mesh):
    return jax.shard_map(
        steps,
        mesh=mesh,
        in_specs=(
            P(None, "wide", "narrow", None),
            P(None, "wide", "narrow", None),
            P("wide", "narrow", None),
            P(),
            P(),
        ),
        out_specs=(
            P("wide", "narrow", None),
            P("wide", "narrow", None),
            P("wide", "narrow", None),
            P("wide", "narrow", None),
            P("wide", "narrow", None),
            P(),
            P(),
        ),
        check_vma=False,
    )
```
